32 devices in a mesh: ka: 4 (over y, x), ga: 8 (over z, core).
Axes of the slice: x: 2, y: 2, z: 4, core: 2. Of those that a mesh axis runs over, the one named last changes fastest.
Arguments:
- orbitals: bfloat16 [8, 8, 2, 32, 1024], P('ka', None, None, 'ga'), may hold values from -6 to 6
- band_counts: int32 [8], replicated, may hold values from 1 to 8, as said below
- pair_slot: int32 [8, 8], replicated, may hold values from 0 to 7
- kernel: float32 [8, 32, 1024], P(None, None, 'ga'), may hold values from 0.2 to 8
Outputs:
- exchange_vectors: float32 [8, 8, 2, 32, 1024], P('ka', None, None, 'ga')
- exchange_matrix: float32 [8, 2, 8, 8], P('ka')
- exchange_energy: float32 [], replicated
The draws below stay inside these ranges and needn't reach their ends.
Inputs may be any that keep to these rules, and one draw needn't show every extreme that they name: The first band_counts[k] band slots of k-point k are the occupied ones; some k-point has all 8 slots occupied.
All inputs are finite; a program needn't handle non-finite values.
Results may differ from the reference program's by a relative error of at most 0.0003.
Values may be sent and summed in bfloat16 or wider, within the bound.
A program may use at most 128 MiB of HBM per device.

```python
import math
import jax
import jax.numpy as jnp
from jax import lax

G = 32
K_DEV = 2
BANDS = 8
STEPS = 2
KPOINTS = 8
N_KA = 4


def draw_band_counts(key, part):
    first_key, second_key, third_key = jax.random.split(key, 3)
    partial_fill = jax.random.randint(first_key, (KPOINTS,), 1, BANDS // 2 + 1)
    full_mark = jax.random.randint(second_key, (KPOINTS,), 0, 4) == 0
    counts = jnp.where(full_mark, BANDS, partial_fill)
    chosen = jax.random.randint(third_key, (), 0, KPOINTS)
    positions = jnp.arange(KPOINTS)
    counts = jnp.where(positions == chosen, BANDS, counts)
    return counts.astype(jnp.int32)


def with_ends(array, own_key, low, top_value):
    longest = array.shape.index(max(array.shape))
    spots = []
    for shift in (0, 1):
        where = [jax.random.randint(jax.random.fold_in(own_key, axis), (), 0, length) for axis, length in enumerate(array.shape)]
        where[longest] = (where[longest] + shift) % array.shape[longest]
        spots.append(tuple(where))
    return array.at[spots[0]].set(low).at[spots[1]].set(top_value)


def level_of(stream_key, extent, cuts, least, high):
    def one(axis_at, parts):
        steps = jax.random.uniform(jax.random.fold_in(jax.random.fold_in(stream_key, 6), axis_at), (parts,), jnp.float32, least / len(cuts), high / len(cuts))
        return jnp.repeat(jnp.exp(steps), extent[axis_at] // parts).reshape((-1,) + (1,) * (len(extent) - axis_at - 1))

    factor_of = one(*cuts[0])
    for cut in cuts[1:]:
        factor_of = factor_of * one(*cut)
    return factor_of


def gaussian(own_key, dims, scale, bound, cuts=(), kind=jnp.bfloat16):
    values = jax.random.normal(own_key, dims, jnp.float32) * scale
    if len(cuts) > 0:
        values = level_of(own_key, dims, cuts, -0.22, 0.18) * values
    return jnp.clip(values, min=-bound, max=bound).astype(kind)


def setup_inputs(seed: int = 0) -> dict:
    keys = jax.random.split(jax.random.key(seed), 5)
    orbitals = gaussian(keys[0], (KPOINTS, BANDS, 2, G, G * G), 1.0, 6.0, ((0, 4), (3, 8)))
    band_counts = draw_band_counts(jax.random.fold_in(keys[4], 71), 0)
    pair_slot = with_ends(jax.random.randint(keys[2], (KPOINTS, KPOINTS), 0, KPOINTS), jax.random.fold_in(keys[2], 1), 0, KPOINTS - 1).astype(jnp.int32)
    kernel = jnp.clip(jnp.exp(math.log(8.0) - 3.6888794 * jax.random.uniform(keys[3], (KPOINTS, G, G * G), jnp.float32) ** level_of(keys[3], (KPOINTS, G, G * G), ((2, 8),), -0.2, 0.2)), 0.2, 8.0)
    return dict(orbitals=orbitals, band_counts=band_counts, pair_slot=pair_slot, kernel=kernel)


highest = lax.Precision.HIGHEST


def contract(first_field, second_field):
    return jnp.einsum("kar,kbr->kab", first_field, second_field, precision=highest)


def reference(orbitals, band_counts, pair_slot, kernel):
    kpoints = orbitals.shape[0]
    band_count = orbitals.shape[1]
    points = orbitals.shape[3]
    volume = points * points * points
    occupied = (jnp.arange(band_count, dtype=jnp.int32)[None, :] < band_counts[:, None]).astype(jnp.float32)
    real_part = orbitals[:, :, 0].astype(jnp.float32)
    imag_part = orbitals[:, :, 1].astype(jnp.float32)
    grid_shape = (kpoints, band_count, points, points, points)
    orbital_field = lax.complex(real_part, imag_part).reshape(grid_shape)
    spectra_kernel = kernel.reshape(kpoints, points, points, points)

    def one_kpoint(kpoint):
        own_group = kpoint // K_DEV
        own_field = orbital_field[kpoint]
        total_real = jnp.zeros((band_count, points, points, points), jnp.float32)
        total_imag = jnp.zeros((band_count, points, points, points), jnp.float32)
        for rotation in range(STEPS):
            anchor = (own_group - rotation) % N_KA
            window = (anchor * K_DEV + jnp.arange(K_DEV, dtype=jnp.int32)).astype(jnp.int32)
            partner = orbital_field[window] * occupied[window][:, :, None, None, None]
            density = jnp.conj(partner)[None] * own_field[:, None, None]
            spectra = jnp.fft.fftn(density, axes=(3, 4, 5))
            chosen = spectra_kernel[pair_slot[kpoint, window]]
            potential = jnp.fft.ifftn(spectra * chosen[None, :, None], axes=(3, 4, 5))
            product_field = jnp.sum(partner[None] * potential, axis=(1, 2))
            total_real = total_real + jnp.real(product_field)
            total_imag = total_imag + jnp.imag(product_field)
        prefactor = -1.0 / kpoints
        stacked = jnp.stack((total_real, total_imag), axis=1)
        return stacked.reshape(band_count, 2, points, points * points) * prefactor

    exchange_vectors = lax.map(one_kpoint, jnp.arange(kpoints, dtype=jnp.int32))
    flat_orbitals = orbitals.astype(jnp.float32).reshape(kpoints, band_count, 2, volume)
    flat_vectors = exchange_vectors.reshape(kpoints, band_count, 2, volume)
    matrix_real = (contract(flat_orbitals[:, :, 0], flat_vectors[:, :, 0]) + contract(flat_orbitals[:, :, 1], flat_vectors[:, :, 1])) / volume
    matrix_imag = (contract(flat_orbitals[:, :, 0], flat_vectors[:, :, 1]) - contract(flat_orbitals[:, :, 1], flat_vectors[:, :, 0])) / volume
    exchange_matrix = jnp.stack((matrix_real, matrix_imag), axis=1)
    exchange_energy = jnp.sum(occupied * jnp.diagonal(matrix_real, axis1=1, axis2=2)) / (2.0 * kpoints)
    return exchange_vectors, exchange_matrix, exchange_energy
```

```python
import functools

import jax
import jax.numpy as jnp
import numpy as np
from jax import lax
from jax.experimental import pallas as pl
from jax.experimental.pallas import tpu as pltpu
from jax.sharding import PartitionSpec as P

LANES = 128
CHUNK = 2
LAG = 5
MESH = pl.DeviceIdType.MESH


def split_np(matrix):
    high = matrix.astype(np.float32).astype(jnp.bfloat16)
    low = (matrix - high.astype(np.float64)).astype(np.float32).astype(jnp.bfloat16)
    return high, low


def real_form(matrix):
    return np.block([[matrix.real, -matrix.imag], [matrix.imag, matrix.real]])


def build_tables(points, members):
    wide = LANES // points
    quads = points // (2 * wide)
    planes = points // members
    dft = np.exp(-2j * np.pi * np.outer(np.arange(points), np.arange(points)) / points)
    member_of = np.arange(members).reshape(members // 2, 2).T.reshape(-1)
    x_of = (member_of[:, None] * planes + np.arange(planes)[None, :]).reshape(members, 1, planes)
    y1_of = np.arange(quads).reshape(1, quads, 1)
    x_of, y1_of = (np.broadcast_to(v, (members, quads, planes)).reshape(-1) for v in (x_of, y1_of))
    gx = np.tile(np.arange(points), quads)
    q = np.repeat(np.arange(quads), points)
    left, left_back = [], []
    for p in range(2):
        phase = np.outer(gx, x_of) / points + np.outer(p + 2 * q, y1_of) * wide / points
        forward = np.exp(-2j * np.pi * phase)
        high, low = split_np(real_form(forward))
        left.append(np.concatenate([high, low, high], axis=1))
        high, low = split_np(real_form(np.conj(forward).T))
        left_back.append(np.concatenate([high, low, high], axis=1))
    small = np.exp(-2j * np.pi * np.outer(np.arange(wide), np.arange(wide)) / wide)
    lane = np.kron(small, dft)
    right = []
    for matrix in (lane, np.conj(lane)):
        high, low = split_np(real_form(matrix).T)
        right.append(np.concatenate([high, low, high], axis=0))
    low_freq = (np.arange(2)[:, None] + 2 * np.arange(quads)[None, :]).reshape(-1)
    y0 = np.repeat(np.arange(wide), points)
    twiddle = np.exp(-2j * np.pi * np.outer(low_freq, y0) / points)
    twiddle = np.stack([twiddle.real, twiddle.imag]).astype(np.float32)
    return np.stack(left), np.stack(left_back), right[0], right[1], twiddle


def split(values):
    high = values.astype(jnp.bfloat16)
    low = (values - high.astype(jnp.float32)).astype(jnp.bfloat16)
    return high, low


def exchange_kernel(dims, counts, slots, pieces, kernel, left_in, left_back_in, right_in, right_back_in, twiddle_in,
                    out, matrix, energy,
                    block, left, left_back, right, right_back, twiddle, staged, raw, multiplier,
                    own, total, arrived, lanes_of, mail, mails, note, notes,
                    table_sem, local_sem, z_send, z_recv, d_send, d_recv, x_send, x_recv, p_send, p_recv,
                    kz_send, kz_recv, kd_send, kd_recv, o_send, o_recv, m_send, m_recv, e_send, e_recv):
    local, bands, members, groups, points, planes = dims
    orbitals = local * bands
    chips = members // 2
    rows = max(1, orbitals // members)
    share = max(1, members // orbitals)
    windows = 2 * local
    steps = orbitals // CHUNK
    wide = LANES // points
    quads = points // (2 * wide)
    tall = quads * points
    piece = tall // members
    held = points // members
    volume = float(points ** 3)
    scale = -1.0 / (groups * local * volume)
    ready = max(1, 2 * rows // CHUNK)

    me = lax.axis_index("ga")
    group = lax.axis_index("ka")
    core, chip = lax.rem(me, 2), lax.div(me, 2)
    partner = chip * 2 + 1 - core
    after = lax.rem(group + 1, groups)

    def row_of(member):
        return lax.div(member, share) * rows

    def start_of(at):
        return lax.div(row_of(at * 2), CHUNK)

    def chunk_of(at, j):
        return pl.ds(lax.rem(start_of(at) + j, steps) * CHUNK, CHUNK)

    first_row = row_of(me)
    own_local = lax.div(first_row, bands)
    window_kpoints = [lax.rem(group + groups - w // local, groups) * local + w % local for w in range(windows)]

    def remote(src, dst, send, recv, **where):
        return pltpu.make_async_remote_copy(src_ref=src, dst_ref=dst, send_sem=send, recv_sem=recv,
                                            device_id=where, device_id_type=MESH)

    table_copies = [pltpu.make_async_copy(src, dst, table_sem.at[i]) for i, (src, dst) in enumerate(
        [(left_in, left), (left_back_in, left_back), (right_in, right), (right_back_in, right_back),
         (twiddle_in, twiddle)])]
    for copy in table_copies:
        copy.start()
    place = pltpu.make_async_copy(pieces, block.at[pl.ds(0, orbitals), core, chip], local_sem.at[0])
    place.start()
    for l in range(local):
        for w in range(windows):
            staged[l, w] = kernel[slots[group * local + l, window_kpoints[w]]] * scale

    barrier = pltpu.get_barrier_semaphore()
    for d in range(1, members):
        pl.semaphore_signal(barrier, inc=1, device_id={"ga": lax.rem(me + d, members)}, device_id_type=MESH)
    for d in range(1, groups):
        pl.semaphore_signal(barrier, inc=1, device_id={"ka": lax.rem(group + d, groups)}, device_id_type=MESH)
    pl.semaphore_wait(barrier, members + groups - 2)

    def z_copy(j, d):
        at = lax.rem(chip + d, chips)
        chunk = chunk_of(at, j)
        return remote(pieces.at[chunk], block.at[chunk, core, chip], z_send.at[d - 1], z_recv.at[j], ga=at * 2 + core)

    def kz_copy(d):
        at = lax.rem(chip + d, chips)
        return remote(staged.at[lax.div(row_of(at * 2), bands)], raw.at[core, chip], kz_send.at[d - 1], kz_recv.at[0],
                      ga=at * 2 + core)

    for d in range(1, chips):
        kz_copy(d).start()

    def z_start(j, carry):
        for d in range(1, chips):
            z_copy(j, d).start()
        return carry

    lax.fori_loop(0, steps, z_start, 0)
    kplace = pltpu.make_async_copy(staged.at[own_local], raw.at[core, chip], local_sem.at[1])
    kplace.start()

    def d_copy(j):
        here = block.at[chunk_of(chip, j), core]
        return remote(here, here, d_send.at[j], d_recv.at[j], ga=partner)

    def x_copy(j):
        chunk = lax.rem(start_of(chip) + j, steps) * CHUNK
        return remote(block.at[pl.ds(chunk, CHUNK), core], block.at[pl.ds(orbitals + chunk, CHUNK), core],
                      x_send.at[j], x_recv.at[j], ka=after)

    def p_copy(j):
        chunk = lax.rem(start_of(chip) + j, steps) * CHUNK
        here = block.at[pl.ds(orbitals + chunk, CHUNK), core]
        return remote(here, here, p_send.at[j], p_recv.at[j], ga=partner)

    def wait_for(dst, sem):
        pltpu.make_async_copy(dst, dst, sem).wait()

    def pass_own(j):
        wait_for(block.at[pl.ds(0, CHUNK), 0, pl.ds(0, chips - 1)], z_recv.at[j])
        d_copy(j).start()
        x_copy(j).start()

    place.wait()
    kplace.wait()
    wait_for(raw.at[0, pl.ds(0, chips - 1)], kz_recv.at[0])
    kd_copy = remote(raw.at[core], raw.at[core], kd_send.at[0], kd_recv.at[0], ga=partner)
    kd_copy.start()
    for j in range(ready):
        pass_own(j)
    for copy in table_copies:
        copy.wait()
    total[...] = jnp.zeros_like(total)
    kd_copy.wait_recv()

    each = points // members
    for w in range(windows):
        for p in range(2):
            for q in range(quads):
                parts = []
                for a in range(wide):
                    gy = a * 2 * quads + 2 * q + p
                    at = gy // each
                    value = raw[at % 2, at // 2, w]
                    parts.append(value[:, (gy % each) * points:(gy % each + 1) * points])
                multiplier[w, (p * quads + q) * points:(p * quads + q + 1) * points, :] = jnp.concatenate(parts, axis=1)

    def load(slot, part, h):
        value = block[slot, :, :, part * 2 + h]
        return value.astype(jnp.float32).reshape(tall, LANES)

    for j in range(ready):
        d_copy(j).wait_recv()
    for r in range(rows):
        for part in range(2):
            for h in range(2):
                own[r, part, h] = load(first_row + r, part, h)

    def rotate(real_part, imag_part, p, sign):
        cos = twiddle[0, p * quads:(p + 1) * quads, :].reshape(quads, 1, LANES)
        sin = twiddle[1, p * quads:(p + 1) * quads, :].reshape(quads, 1, LANES) * sign
        real_part = real_part.reshape(quads, points, LANES)
        imag_part = imag_part.reshape(quads, points, LANES)
        new_real = real_part * cos - imag_part * sin
        new_imag = imag_part * cos + real_part * sin
        return new_real.reshape(tall, LANES), new_imag.reshape(tall, LANES)

    def dot(a, b):
        return jnp.dot(a, b, preferred_element_type=jnp.float32)

    def from_left(table, values):
        high, low = split(values)
        return dot(table, jnp.concatenate([high, high, low], axis=0))

    def from_right(values, table):
        high, low = split(values)
        return dot(jnp.concatenate([high, high, low], axis=1), table)

    def partner_body(i, carry):
        step = lax.div(i, CHUNK)
        fresh = lax.rem(i, CHUNK) == 0

        @pl.when(fresh & (step + ready < steps))
        def _():
            pass_own(step + ready)

        @pl.when(fresh & (step >= LAG) & (step < steps + LAG))
        def _():
            j = step - LAG
            x_copy(j).wait_recv()
            p_copy(j).start()

        @pl.when(fresh & (step >= ready) & (step < steps))
        def _():
            d_copy(step).wait_recv()

        @pl.when(fresh & (step >= steps))
        def _():
            p_copy(step - steps).wait_recv()

        back = lax.div(step, steps)
        orbital = lax.rem(start_of(chip) + lax.rem(step, steps), steps) * CHUNK + lax.rem(i, CHUNK)
        slot = back * orbitals + orbital
        at_local, band = lax.div(orbital, bands), lax.rem(orbital, bands)
        w = back * local + at_local
        kpoint = lax.rem(group + groups - back, groups) * local + at_local
        keep = jnp.where(band < counts[kpoint], 1.0, 0.0).astype(jnp.float32)
        if share > 1:
            keep = keep * jnp.where(lax.rem(w, share) == lax.rem(me, share), 1.0, 0.0).astype(jnp.float32)
        other = [[load(slot, part, h) * keep for h in range(2)] for part in range(2)]
        inputs = ([], [])
        for r in range(rows):
            fields = []
            for h in range(2):
                real_part = own[r, 0, h] * other[0][h] + own[r, 1, h] * other[1][h]
                imag_part = own[r, 1, h] * other[0][h] - own[r, 0, h] * other[1][h]
                fields.append(jnp.concatenate([real_part, imag_part], axis=0))
            inputs[0].append(fields[0] + fields[1])
            inputs[1].append(fields[0] - fields[1])
        turned = []
        for p in range(2):
            spectrum = from_left(left[p], jnp.concatenate(inputs[p], axis=1))
            for r in range(rows):
                cut = spectrum[:, r * LANES:(r + 1) * LANES]
                turned.append(jnp.concatenate(rotate(cut[:tall], cut[tall:], p, 1.0), axis=1))
        full = from_right(jnp.concatenate(turned, axis=0), right[...])
        weighted = []
        for p in range(2):
            chosen = multiplier[w, p * tall:(p + 1) * tall, :]
            chosen = jnp.concatenate([chosen, chosen], axis=1)
            for r in range(rows):
                n = p * rows + r
                weighted.append(full[n * tall:(n + 1) * tall] * chosen)
        full = from_right(jnp.concatenate(weighted, axis=0), right_back[...])
        halves = []
        for p in range(2):
            back_p = []
            for r in range(rows):
                n = p * rows + r
                cut = full[n * tall:(n + 1) * tall]
                back_p.append(jnp.concatenate(rotate(cut[:, :LANES], cut[:, LANES:], p, -1.0), axis=0))
            halves.append(from_left(left_back[p], jnp.concatenate(back_p, axis=1)))
        for h in range(2):
            potential = halves[0] + halves[1] if h == 0 else halves[0] - halves[1]
            for r in range(rows):
                real_part = potential[:tall, r * LANES:(r + 1) * LANES]
                imag_part = potential[tall:, r * LANES:(r + 1) * LANES]
                total[r, 0, h] += other[0][h] * real_part - other[1][h] * imag_part
                total[r, 1, h] += other[0][h] * imag_part + other[1][h] * real_part
        return carry

    lax.fori_loop(0, 2 * orbitals, partner_body, 0)

    def seat(member):
        return lax.rem(member, 2) * chips + lax.div(member, 2)

    def o_copy(d):
        to = lax.rem(me + d, members)
        return remote(total.at[:, :, :, pl.ds(pl.multiple_of(seat(to) * piece, piece), piece)],
                      arrived.at[lax.rem(me, share), pl.ds(first_row, rows)], o_send.at[d - 1], o_recv.at[d - 1], ga=to)

    for d in range(1, members):
        o_copy(d).start()

    def project(a, carry):
        for r in range(rows):
            real_sum = jnp.zeros((tall, LANES), jnp.float32)
            imag_sum = jnp.zeros((tall, LANES), jnp.float32)
            for h in range(2):
                first, second = load(own_local * bands + a, 0, h), load(own_local * bands + a, 1, h)
                real_sum += first * total[r, 0, h] + second * total[r, 1, h]
                imag_sum += first * total[r, 1, h] - second * total[r, 0, h]
            lanes_of[r, 0, pl.ds(a, 1)] = jnp.sum(real_sum, axis=0, keepdims=True)
            lanes_of[r, 1, pl.ds(a, 1)] = jnp.sum(imag_sum, axis=0, keepdims=True)
        return carry

    lax.fori_loop(0, bands, project, 0)
    lane = lax.broadcasted_iota(jnp.int32, (bands, LANES), 1)
    level = lax.broadcasted_iota(jnp.int32, (bands, LANES), 0)
    entry = 2 * local * bands
    letter = jnp.zeros((bands, LANES), jnp.float32)
    for r in range(rows):
        at_band = lax.rem(first_row, bands) + r
        filled = jnp.where(at_band < counts[group * local + own_local], 1.0, 0.0).astype(jnp.float32)
        for part in range(2):
            value = jnp.sum(lanes_of[r, part], axis=1, keepdims=True) / volume
            letter = jnp.where(lane == (own_local * 2 + part) * bands + at_band, value, letter)
            if part == 0:
                term = jnp.where(level == at_band, value, 0.0) * (filled / (2.0 * groups * local))
                letter = letter + jnp.where(lane == entry, term, 0.0)
    mail[...] = letter
    mails[me] = letter

    def m_copy(d):
        to = lax.rem(me + d, members)
        return remote(mail, mails.at[me], m_send.at[d - 1], m_recv.at[d - 1], ga=to)

    for d in range(1, members):
        m_copy(d).start()

    own_part = pltpu.make_async_copy(total.at[:, :, :, pl.ds(pl.multiple_of(seat(me) * piece, piece), piece)],
                                     arrived.at[lax.rem(me, share), pl.ds(first_row, rows)], local_sem.at[2])
    own_part.start()
    for d in range(1, members):
        m_copy(d).wait_recv()
    summed = jnp.sum(mails[...], axis=0)
    for l in range(local):
        for part in range(2):
            begin = (l * 2 + part) * bands
            matrix[l, part] = summed[:, begin:begin + bands]
    mine = jnp.where(lane == entry, summed, 0.0)
    note[...] = mine
    notes[group] = mine

    def e_copy(d):
        to = lax.rem(group + d, groups)
        return remote(note, notes.at[group], e_send.at[d - 1], e_recv.at[d - 1], ka=to)

    for d in range(1, groups):
        e_copy(d).start()

    own_part.wait()
    for d in range(1, members):
        o_copy(d).wait_recv()

    def place_out(o, carry):
        l, b = lax.div(o, bands), lax.rem(o, bands)
        for part in range(2):
            for h in range(2):
                value = arrived[0, o, part, h]
                for n in range(1, share):
                    value = value + arrived[n, o, part, h]
                for y in range(quads):
                    t = h * quads + y
                    out[l, b, part, :, t * LANES:(t + 1) * LANES] = value[y * held:(y + 1) * held]
        return carry

    lax.fori_loop(0, orbitals, place_out, 0)
    for d in range(1, groups):
        e_copy(d).wait_recv()
    energy[0, 0] = jnp.sum(notes[...])

    for d in range(1, chips):
        wait_for(pieces, z_send.at[d - 1])
        kz_copy(d).wait_send()
    kd_copy.wait_send()

    def drain(j, carry):
        d_copy(j).wait_send()
        x_copy(j).wait_send()
        p_copy(j).wait_send()
        return carry

    lax.fori_loop(0, steps, drain, 0)
    for d in range(1, members):
        o_copy(d).wait_send()
        m_copy(d).wait_send()
    for d in range(1, groups):
        e_copy(d).wait_send()


def on_device(orbitals, band_counts, pair_slot, kernel):
    local, bands, _, planes, columns = orbitals.shape
    slots, points, width = kernel.shape
    members = lax.axis_size("ga")
    groups = lax.axis_size("ka")
    wide = LANES // points
    quads = points // (2 * wide)
    tall = quads * points
    tiles = columns // LANES
    count = local * bands
    rows = max(1, count // members)
    share = max(1, members // count)
    windows = 2 * local
    piece = tall // members
    steps = count // CHUNK
    chips = members // 2
    tables = build_tables(points, members)
    f32, bf16 = jnp.float32, jnp.bfloat16

    pieces = orbitals.reshape(count, 2, planes, tiles, LANES).transpose(0, 1, 3, 2, 4)
    pieces = pieces.reshape(count, 4, piece, LANES)

    smem = pl.BlockSpec(memory_space=pltpu.SMEM)
    vmem = pl.BlockSpec(memory_space=pltpu.VMEM)
    anywhere = pl.BlockSpec(memory_space=pl.ANY)
    dims = (local, bands, members, groups, points, planes)
    dma = pltpu.SemaphoreType.DMA
    out, matrix, energy = pl.pallas_call(
        functools.partial(exchange_kernel, dims),
        out_shape=(jax.ShapeDtypeStruct((local, bands, 2, planes, columns), f32),
                   jax.ShapeDtypeStruct((local, 2, bands, bands), f32),
                   jax.ShapeDtypeStruct((1, 1), f32)),
        in_specs=[smem, smem, vmem, vmem] + [anywhere] * 5,
        out_specs=(vmem, vmem, smem),
        scratch_shapes=[
            pltpu.VMEM((2 * count, 2, chips, 4, piece, LANES), bf16),
            pltpu.VMEM(tables[0].shape, bf16), pltpu.VMEM(tables[1].shape, bf16),
            pltpu.VMEM(tables[2].shape, bf16), pltpu.VMEM(tables[3].shape, bf16),
            pltpu.VMEM(tables[4].shape, f32),
            pltpu.VMEM((local, windows, points, width), f32),
            pltpu.VMEM((2, chips, windows, points, width), f32),
            pltpu.VMEM((windows, 2 * tall, LANES), f32),
            pltpu.VMEM((rows, 2, 2, tall, LANES), f32),
            pltpu.VMEM((rows, 2, 2, tall, LANES), f32),
            pltpu.VMEM((share, count, 2, 2, piece, LANES), f32),
            pltpu.VMEM((rows, 2, bands, LANES), f32),
            pltpu.VMEM((bands, LANES), f32),
            pltpu.VMEM((members, bands, LANES), f32),
            pltpu.VMEM((bands, LANES), f32),
            pltpu.VMEM((groups, bands, LANES), f32),
            dma((5,)), dma((3,)),
            dma((chips - 1,)), dma((steps,)), dma((steps,)), dma((steps,)), dma((steps,)), dma((steps,)),
            dma((steps,)), dma((steps,)),
            dma((chips - 1,)), dma((1,)), dma((1,)), dma((1,)),
            dma((members - 1,)), dma((members - 1,)), dma((members - 1,)), dma((members - 1,)),
            dma((groups - 1,)), dma((groups - 1,)),
        ],
        compiler_params=pltpu.CompilerParams(vmem_limit_bytes=56 * 2 ** 20, collective_id=0, has_side_effects=True),
        name="exchange",
    )(band_counts, pair_slot, pieces, kernel, *[jnp.asarray(table) for table in tables])
    return out, matrix, energy.reshape(())


def solution(mesh):
    in_specs = (P("ka", None, None, "ga", None), P(), P(), P(None, None, "ga"))
    out_specs = (P("ka", None, None, "ga", None), P("ka", None, None, None), P())
    return jax.shard_map(
        on_device, mesh=mesh, in_specs=in_specs, out_specs=out_specs, check_vma=False
    )
```

```python
import functools

import jax
import jax.numpy as jnp
import numpy as np
from jax import lax
from jax.experimental import pallas as pl
from jax.experimental.pallas import tpu as pltpu
from jax.sharding import PartitionSpec as P

LANES = 128
RADIX = 4
CHUNK = 2
LEAD = 3
SPLIT = 6
MESH = pl.DeviceIdType.MESH


def split_np(matrix):
    high = matrix.astype(np.float32).astype(jnp.bfloat16)
    low = (matrix - high.astype(np.float64)).astype(np.float32).astype(jnp.bfloat16)
    return high, low


def real_form(matrix):
    return np.block([[matrix.real, -matrix.imag], [matrix.imag, matrix.real]])


def build_tables(points, members):
    wide = LANES // points
    quads = points // (2 * wide)
    planes = points // members
    dft = np.exp(-2j * np.pi * np.outer(np.arange(points), np.arange(points)) / points)
    member_of = np.arange(members).reshape(members // 2, 2).T.reshape(-1)
    x_of = (member_of[:, None] * planes + np.arange(planes)[None, :]).reshape(members, 1, planes)
    deep = 2 * quads // RADIX
    b_of = np.arange(deep).reshape(1, deep, 1)
    x_of, b_of = (np.broadcast_to(v, (members, deep, planes)).reshape(-1) for v in (x_of, b_of))
    gx = np.tile(np.arange(points), deep)
    high_freq = np.repeat(np.arange(deep), points)
    left, left_back = [], []
    for c in range(RADIX):
        phase = np.outer(gx, x_of) / points + np.outer(c + RADIX * high_freq, b_of) / (2 * quads)
        forward = np.exp(-2j * np.pi * phase)
        high, low = split_np(real_form(forward))
        left.append(np.concatenate([high, high, low], axis=1))
        high, low = split_np(real_form(np.conj(forward).T))
        left_back.append(np.concatenate([high, high, low], axis=1))
    small = np.exp(-2j * np.pi * np.outer(np.arange(wide), np.arange(wide)) / wide)
    lane = np.kron(small, dft)
    right = []
    for matrix in (lane, np.conj(lane)):
        high, low = split_np(real_form(matrix).T)
        right.append(np.concatenate([high, low, high], axis=0))
    low_freq = (np.arange(RADIX)[:, None] + RADIX * np.arange(deep)[None, :]).reshape(-1)
    y0 = np.repeat(np.arange(wide), points)
    twiddle = np.exp(-2j * np.pi * np.outer(low_freq, y0) / points)
    twiddle = np.stack([twiddle.real, twiddle.imag]).astype(np.float32)
    return np.stack(left), np.stack(left_back), right[0], right[1], twiddle


def split(values):
    high = values.astype(jnp.bfloat16)
    low = (values - high.astype(jnp.float32)).astype(jnp.bfloat16)
    return high, low


def exchange_kernel(dims, counts, slots, pieces, kernel, left_in, left_back_in, right_in, right_back_in, twiddle_in,
                    out, matrix, energy,
                    block, left, left_back, right, right_back, twiddle, staged, raw, multiplier,
                    own, total, arrived, lanes_of, mail, mails, note, notes,
                    table_sem, local_sem, z_send, z_recv, r_send, d_send, d_recv, xo_send, xo_recv, x_send, x_recv,
                    p_send, p_recv, kz_send, kz_recv, kd_send, kd_recv, o_send, o_recv, m_send, m_recv, e_send, e_recv):
    local, bands, members, groups, points, planes = dims
    orbitals = local * bands
    chips = members // 2
    rows = max(1, orbitals // members)
    share = max(1, members // orbitals)
    landing = out if share == 1 else arrived
    windows = 2 * local
    steps = orbitals // CHUNK
    wide = LANES // points
    quads = points // (2 * wide)
    tall = quads * points
    deep = 2 * quads // RADIX
    low = deep * points
    piece = tall // members
    held = points // members
    volume = float(points ** 3)
    scale = -1.0 / (groups * local * volume)
    ready = max(1, 2 * rows // CHUNK)
    lead = min(max(LEAD, ready), steps)
    late = SPLIT if rows > 1 else 0
    paired = steps - max(late, lead)
    turns = 2 * steps - late
    relayed = 2 < chips <= 4

    me = lax.axis_index("ga")
    group = lax.axis_index("ka")
    core, chip = lax.rem(me, 2), lax.div(me, 2)
    partner = chip * 2 + 1 - core
    after = lax.rem(group + 1, groups)

    def row_of(member):
        return lax.div(member, share) * rows

    def start_of(at):
        return lax.div(row_of(at * 2), CHUNK)

    def chunk_at(at, j):
        rising = lax.rem(start_of(at) + j, steps)
        falling = lax.rem(start_of(at) + ready - 1 - j + 2 * steps, steps)
        return jnp.where(at < chips // 2, rising, falling) * CHUNK

    def chunk_of(at, j):
        return pl.ds(chunk_at(at, j), CHUNK)

    first_row = row_of(me)
    own_local = lax.div(first_row, bands)
    window_kpoints = [lax.rem(group + groups - w // local, groups) * local + w % local for w in range(windows)]

    def remote(src, dst, send, recv, **where):
        return pltpu.make_async_remote_copy(src_ref=src, dst_ref=dst, send_sem=send, recv_sem=recv,
                                            device_id=where, device_id_type=MESH)

    table_copies = [pltpu.make_async_copy(src, dst, table_sem.at[i]) for i, (src, dst) in enumerate(
        [(left_in, left), (left_back_in, left_back), (right_in, right), (right_back_in, right_back),
         (twiddle_in, twiddle)])]
    for copy in table_copies:
        copy.start()
    place = pltpu.make_async_copy(pieces, block.at[pl.ds(0, orbitals), core, chip], local_sem.at[0])
    place.start()
    for l in range(local):
        for w in range(windows):
            staged[l, w] = kernel[slots[group * local + l, window_kpoints[w]]] * scale

    barrier = pltpu.get_barrier_semaphore()
    for d in range(1, members):
        pl.semaphore_signal(barrier, inc=1, device_id={"ga": lax.rem(me + d, members)}, device_id_type=MESH)
    for d in range(1, groups):
        pl.semaphore_signal(barrier, inc=1, device_id={"ka": lax.rem(group + d, groups)}, device_id_type=MESH)
    pl.semaphore_wait(barrier, members + groups - 2)

    offsets = [d for d in range(1 - chips, chips) if d != 0]
    ordered = sorted(offsets, key=lambda d: -abs(d))

    def z_copy(j, d):
        chunk = chunk_of(chip + d, j)
        return remote(pieces.at[chunk], block.at[chunk, core, chip], z_send.at[offsets.index(d)], z_recv.at[j],
                      ga=(chip + d) * 2 + core)

    def inside(d):
        return (chip + d >= 0) & (chip + d < chips)

    def far(d):
        return relayed and abs(d) == chips - 1

    def z_start(j, stop):
        for d in ordered:
            @pl.when(inside(d) & (j < (ready if far(d) else steps)))
            def _():
                z_copy(j, d).start()
        return stop

    def kz_copy(half, d):
        at = lax.rem(chip + d, chips)
        part = pl.ds(half * local, local)
        return remote(staged.at[lax.div(row_of(at * 2), bands), part], raw.at[half, core, chip],
                      kz_send.at[half, d - 1], kz_recv.at[half], ga=at * 2 + core)

    def relay_copy(j):
        low = chip == 1
        end, origin = jnp.where(low, 0, chips - 1), jnp.where(low, chips - 1, 0)
        chunk = chunk_of(end, j)
        here = block.at[chunk, core, origin]
        return remote(here, here, r_send.at[0], z_recv.at[j], ga=end * 2 + core)

    xo_copy = remote(pieces, block.at[pl.ds(orbitals, orbitals), core, chip], xo_send.at[0], xo_recv.at[0], ka=after)
    for j in range(ready):
        z_start(j, 0)
    for d in range(1, chips):
        kz_copy(0, d).start()
    xo_copy.start()
    for j in range(ready, lead):
        z_start(j, 0)
    for d in range(1, chips):
        kz_copy(1, d).start()
    lax.fori_loop(lead, steps, z_start, 0)
    kplaces = [pltpu.make_async_copy(staged.at[own_local, pl.ds(half * local, local)], raw.at[half, core, chip],
                                     local_sem.at[1 + half]) for half in range(2)]
    for copy in kplaces:
        copy.start()

    def d_copy(j):
        here = block.at[chunk_of(chip, j), core]
        return remote(here, here, d_send.at[j], d_recv.at[j], ga=partner)

    def x_copy(j, d):
        chunk = chunk_at(chip, j)
        at = lax.rem(chip + d, chips)
        return remote(block.at[pl.ds(chunk, CHUNK), core, at], block.at[pl.ds(orbitals + chunk, CHUNK), core, at],
                      x_send.at[d - 1], x_recv.at[j], ka=after)

    def p_copy(j):
        chunk = chunk_at(chip, j)
        here = block.at[pl.ds(orbitals + chunk, CHUNK), core]
        return remote(here, here, p_send.at[j], p_recv.at[j], ga=partner)

    def wait_for(dst, sem):
        pltpu.make_async_copy(dst, dst, sem).wait()

    def arrived_z(sem):
        wait_for(block.at[pl.ds(0, CHUNK), 0, pl.ds(0, chips - 1)], sem)

    def pass_own(j):
        arrived_z(z_recv.at[j])
        if relayed:
            @pl.when(((chip == 1) | (chip == chips - 2)) & (j + ready < steps))
            def _():
                relay_copy(j + ready).start()
        d_copy(j).start()
        for d in range(1, chips):
            x_copy(j, d).start()

    def kd_copy(half):
        return remote(raw.at[half, core], raw.at[half, core], kd_send.at[half], kd_recv.at[half], ga=partner)

    def pass_kernel(half):
        kplaces[half].wait()
        wait_for(raw.at[half, 0, pl.ds(0, chips - 1)], kz_recv.at[half])
        kd_copy(half).start()

    place.wait()
    for j in range(ready):
        pass_own(j)
    pass_kernel(0)
    for copy in table_copies:
        copy.wait()
    total[...] = jnp.zeros_like(total)

    each = points // members

    def lay_out(half):
        kd_copy(half).wait_recv()
        for l in range(local):
            for c in range(RADIX):
                for q in range(deep):
                    parts = []
                    for a in range(wide):
                        gy = a * 2 * quads + c + RADIX * q
                        at = gy // each
                        value = raw[half, at % 2, at // 2, l]
                        parts.append(value[:, (gy % each) * points:(gy % each + 1) * points])
                    multiplier[half * local + l, (c * deep + q) * points:(c * deep + q + 1) * points, :] = (
                        jnp.concatenate(parts, axis=1))

    lay_out(0)

    def load(slot, part, h):
        value = block[slot, :, :, part * 2 + h]
        return value.astype(jnp.float32).reshape(tall, LANES)

    for j in range(ready):
        d_copy(j).wait_recv()
    for r in range(rows):
        for part in range(2):
            for h in range(2):
                own[r, part, h] = load(first_row + r, part, h)

    def rotate(real_part, imag_part, c, sign):
        cos = twiddle[0, c * deep:(c + 1) * deep, :].reshape(deep, 1, LANES)
        sin = twiddle[1, c * deep:(c + 1) * deep, :].reshape(deep, 1, LANES) * sign
        real_part = real_part.reshape(deep, points, LANES)
        imag_part = imag_part.reshape(deep, points, LANES)
        new_real = real_part * cos - imag_part * sin
        new_imag = imag_part * cos + real_part * sin
        return new_real.reshape(low, LANES), new_imag.reshape(low, LANES)

    def quarters(value):
        value = value.reshape(members, 2, piece // 2, LANES)
        return [value[:, n].reshape(low, LANES) for n in range(2)]

    def joined(first, second):
        shape = (members, 1, piece // 2, LANES)
        return jnp.concatenate([first.reshape(shape), second.reshape(shape)], axis=1).reshape(tall, LANES)

    def dot(a, b):
        return jnp.dot(a, b, preferred_element_type=jnp.float32)

    def from_left(table, values):
        high, low = split(values)
        return dot(table, jnp.concatenate([high, low, high], axis=0))

    def from_right(values, table):
        high, low = split(values)
        return dot(jnp.concatenate([high, high, low], axis=1), table)

    def turn_of(t):
        u = t - lead
        middle = (u >= 0) & (u < 2 * paired)
        back = jnp.where(middle, 1 - lax.rem(jnp.maximum(u, 0), 2), jnp.where(t - paired < steps, 0, 1))
        half = lax.div(jnp.maximum(u, 0), 2)
        index = jnp.where(u < 0, t, jnp.where(middle, jnp.where(back == 1, half, lead + half),
                                              jnp.where(t - paired < steps, t - paired, t - steps)))
        return back, index

    def partner_of(back, index, i):
        orbital = chunk_at(chip, index) + i
        slot = back * orbitals + orbital
        at_local, band = lax.div(orbital, bands), lax.rem(orbital, bands)
        w = back * local + at_local
        kpoint = lax.rem(group + groups - back, groups) * local + at_local
        keep = jnp.where(band < counts[kpoint], 1.0, 0.0).astype(jnp.float32)
        if share > 1:
            keep = keep * jnp.where(lax.rem(w, share) == lax.rem(me, share), 1.0, 0.0).astype(jnp.float32)
        return slot, w, keep

    def loads(item):
        held_ = {}
        for (slot, _, _), _ in item:
            if id(slot) not in held_:
                held_[id(slot)] = [[load(slot, part, h) for h in range(2)] for part in range(2)]
        return [held_[id(slot)] for (slot, _, _), _ in item]

    def first_stage(item):
        inputs = [[] for _ in range(RADIX)]
        for other, (_, r) in zip(loads(item), item):
            real, imag = [], []
            for h in range(2):
                real += quarters(own[r, 0, h] * other[0][h] + own[r, 1, h] * other[1][h])
                imag += quarters(own[r, 1, h] * other[0][h] - own[r, 0, h] * other[1][h])
            even = [[v[0] + v[2], v[1] + v[3]] for v in (real, imag)]
            odd = [[v[0] - v[2], v[1] - v[3]] for v in (real, imag)]
            inputs[0].append(jnp.concatenate([even[0][0] + even[0][1], even[1][0] + even[1][1]], axis=0))
            inputs[2].append(jnp.concatenate([even[0][0] - even[0][1], even[1][0] - even[1][1]], axis=0))
            inputs[1].append(jnp.concatenate([odd[0][0] + odd[1][1], odd[1][0] - odd[0][1]], axis=0))
            inputs[3].append(jnp.concatenate([odd[0][0] - odd[1][1], odd[1][0] + odd[0][1]], axis=0))
        return [from_left(left[c], jnp.concatenate(inputs[c], axis=1)) for c in range(RADIX)]

    def second_stage(spectra):
        result = []
        for p in range(2):
            turned = []
            for c in range(p * RADIX // 2, (p + 1) * RADIX // 2):
                for n in range(spectra[c].shape[1] // LANES):
                    cut = spectra[c][:, n * LANES:(n + 1) * LANES]
                    turned.append(jnp.concatenate(rotate(cut[:low], cut[low:], c, 1.0), axis=1))
            result.append(from_right(jnp.concatenate(turned, axis=0), right[...]))
        return result

    def third_stage(item, full):
        result = []
        for p in range(2):
            weighted = []
            for n in range(RADIX // 2):
                c = p * RADIX // 2 + n
                chosen = {}
                for i, ((slot, w, keep), _) in enumerate(item):
                    if id(slot) not in chosen:
                        value = multiplier[w, c * low:(c + 1) * low, :] * keep
                        chosen[id(slot)] = jnp.concatenate([value, value], axis=1)
                    at = n * len(item) + i
                    weighted.append(full[p][at * low:(at + 1) * low] * chosen[id(slot)])
            result.append(from_right(jnp.concatenate(weighted, axis=0), right_back[...]))
        return result

    def fourth_stage(item, full):
        values = []
        for p in range(2):
            for n in range(RADIX // 2):
                c = p * RADIX // 2 + n
                back_c = []
                for i in range(len(item)):
                    at = n * len(item) + i
                    cut = full[p][at * low:(at + 1) * low]
                    back_c.append(jnp.concatenate(rotate(cut[:, :LANES], cut[:, LANES:], c, -1.0), axis=0))
                values.append(from_left(left_back[c], jnp.concatenate(back_c, axis=1)))
        return values

    def last_stage(item, values):
        for i, (other, (_, r)) in enumerate(zip(loads(item), item)):
            cut = [value[:, i * LANES:(i + 1) * LANES] for value in values]
            real, imag = [v[:low] for v in cut], [v[low:] for v in cut]
            even = [[v[0] + v[2], v[1] + v[3]] for v in (real, imag)]
            odd = [[v[0] - v[2], v[1] - v[3]] for v in (real, imag)]
            real = [even[0][0] + even[0][1], odd[0][0] - odd[1][1], even[0][0] - even[0][1], odd[0][0] + odd[1][1]]
            imag = [even[1][0] + even[1][1], odd[1][0] + odd[0][1], even[1][0] - even[1][1], odd[1][0] - odd[0][1]]
            for h in range(2):
                real_part = joined(real[2 * h], real[2 * h + 1])
                imag_part = joined(imag[2 * h], imag[2 * h + 1])
                total[r, 0, h] += other[0][h] * real_part - other[1][h] * imag_part
                total[r, 1, h] += other[0][h] * imag_part + other[1][h] * real_part

    def work(a, b):
        va = first_stage(a)
        vb = first_stage(b)
        va = second_stage(va)
        vb = second_stage(vb)
        va = third_stage(a, va)
        vb = third_stage(b, vb)
        va = fourth_stage(a, va)
        vb = fourth_stage(b, vb)
        last_stage(a, va)
        last_stage(b, vb)

    def pass_back(j):
        wait_for(block.at[pl.ds(0, CHUNK), 0, pl.ds(0, chips - 1)], x_recv.at[j])
        p_copy(j).start()

    def step_body(step, carry):
        back, index = turn_of(step)
        next_back, next_index = turn_of(step + 1)

        @pl.when((next_back == 0) & (next_index >= ready))
        def _():
            pass_own(next_index)

        @pl.when(step == lead - 1)
        def _():
            xo_copy.wait_recv()
            pass_kernel(1)

        @pl.when((next_back == 1) & (step + 1 < turns))
        def _():
            pass_back(next_index)

        if late:
            @pl.when((step >= turns - late + 1) & (step + 1 < turns + late))
            def _():
                pass_back(step - turns + late - 1 + steps - late)

        @pl.when((back == 0) & (index >= ready))
        def _():
            d_copy(index).wait_recv()

        @pl.when(step == lead)
        def _():
            lay_out(1)

        @pl.when(back == 1)
        def _():
            p_copy(index).wait_recv()

        partners = [partner_of(back, index, i) for i in range(CHUNK)]
        work(*[[(partner, r) for r in range(rows)] for partner in partners])
        return carry

    lax.fori_loop(0, turns, step_body, 0)

    def seat(member):
        return lax.rem(member, 2) * chips + lax.div(member, 2)

    def o_copy(d, r):
        to = lax.rem(me + d, members)
        return remote(total.at[r, :, :, pl.ds(pl.multiple_of(seat(to) * piece, piece), piece)],
                      landing.at[lax.rem(me, share) * orbitals + first_row + r], o_send.at[r, d - 1], o_recv.at[r, d - 1],
                      ga=to)

    if late:
        pass_back(steps - 1)

    def row_body(r, carry):
        def turn(q, carry):
            first = steps - late + q * 2

            @pl.when(r == 0)
            def _():
                for n in range(2):
                    p_copy(first + n).wait_recv()

            partners = [[partner_of(1, first + n, i) for i in range(CHUNK)] for n in range(2)]
            work(*[[(partner, r) for partner in pair] for pair in partners])
            return carry

        lax.fori_loop(0, late // 2, turn, 0)
        for d in range(1, members):
            o_copy(d, r).start()
        return carry

    if late:
        lax.fori_loop(0, rows, row_body, 0)
    else:
        for r in range(rows):
            for d in range(1, members):
                o_copy(d, r).start()

    def project(a, carry):
        for r in range(rows):
            real_sum = jnp.zeros((tall, LANES), jnp.float32)
            imag_sum = jnp.zeros((tall, LANES), jnp.float32)
            for h in range(2):
                first, second = load(own_local * bands + a, 0, h), load(own_local * bands + a, 1, h)
                real_sum += first * total[r, 0, h] + second * total[r, 1, h]
                imag_sum += first * total[r, 1, h] - second * total[r, 0, h]
            lanes_of[r, 0, pl.ds(a, 1)] = jnp.sum(real_sum, axis=0, keepdims=True)
            lanes_of[r, 1, pl.ds(a, 1)] = jnp.sum(imag_sum, axis=0, keepdims=True)
        return carry

    lax.fori_loop(0, bands, project, 0)
    lane = lax.broadcasted_iota(jnp.int32, (bands, LANES), 1)
    level = lax.broadcasted_iota(jnp.int32, (bands, LANES), 0)
    entry = 2 * local * bands
    letter = jnp.zeros((bands, LANES), jnp.float32)
    for r in range(rows):
        at_band = lax.rem(first_row, bands) + r
        filled = jnp.where(at_band < counts[group * local + own_local], 1.0, 0.0).astype(jnp.float32)
        for part in range(2):
            value = jnp.sum(lanes_of[r, part], axis=1, keepdims=True) / volume
            letter = jnp.where(lane == (own_local * 2 + part) * bands + at_band, value, letter)
            if part == 0:
                term = jnp.where(level == at_band, value, 0.0) * (filled / (2.0 * groups * local))
                letter = letter + jnp.where(lane == entry, term, 0.0)
    mail[...] = letter
    mails[me] = letter

    def m_copy(d):
        to = lax.rem(me + d, members)
        return remote(mail, mails.at[me], m_send.at[d - 1], m_recv.at[d - 1], ga=to)

    for d in range(1, members):
        m_copy(d).start()

    own_part = pltpu.make_async_copy(total.at[:, :, :, pl.ds(pl.multiple_of(seat(me) * piece, piece), piece)],
                                     landing.at[pl.ds(lax.rem(me, share) * orbitals + first_row, rows)], local_sem.at[3])
    own_part.start()
    for d in range(1, members):
        m_copy(d).wait_recv()
    summed = jnp.sum(mails[...], axis=0)
    for l in range(local):
        for part in range(2):
            begin = (l * 2 + part) * bands
            matrix[l, part] = summed[:, begin:begin + bands]
    mine = jnp.where(lane == entry, summed, 0.0)
    note[...] = mine
    notes[group] = mine

    def e_copy(d):
        to = lax.rem(group + d, groups)
        return remote(note, notes.at[group], e_send.at[d - 1], e_recv.at[d - 1], ka=to)

    for d in range(1, groups):
        e_copy(d).start()

    own_part.wait()
    for r in range(rows):
        for d in range(1, members):
            o_copy(d, r).wait_recv()

    if share > 1:
        def add_up(o, carry):
            value = arrived[o]
            for n in range(1, share):
                value = value + arrived[n * orbitals + o]
            out[o] = value
            return carry

        lax.fori_loop(0, orbitals, add_up, 0)
    for d in range(1, groups):
        e_copy(d).wait_recv()
    energy[0, 0] = jnp.sum(notes[...])

    for d in offsets:
        @pl.when(inside(d))
        def _():
            wait_for(pieces.at[pl.ds(0, ready * CHUNK)] if far(d) else pieces, z_send.at[offsets.index(d)])
    if relayed:
        @pl.when((chip == 1) | (chip == chips - 2))
        def _():
            wait_for(pieces.at[pl.ds(0, (steps - ready) * CHUNK)], r_send.at[0])
    for d in range(1, chips):
        wait_for(pieces, x_send.at[d - 1])
        kz_copy(0, d).wait_send()
        kz_copy(1, d).wait_send()
    kd_copy(0).wait_send()
    kd_copy(1).wait_send()
    xo_copy.wait_send()

    def drain(j, carry):
        d_copy(j).wait_send()
        p_copy(j).wait_send()
        return carry

    lax.fori_loop(0, steps, drain, 0)
    for d in range(1, members):
        for r in range(rows):
            o_copy(d, r).wait_send()
        m_copy(d).wait_send()
    for d in range(1, groups):
        e_copy(d).wait_send()


def on_device(orbitals, band_counts, pair_slot, kernel):
    local, bands, _, planes, columns = orbitals.shape
    slots, points, width = kernel.shape
    members = lax.axis_size("ga")
    groups = lax.axis_size("ka")
    wide = LANES // points
    quads = points // (2 * wide)
    tall = quads * points
    tiles = columns // LANES
    count = local * bands
    rows = max(1, count // members)
    share = max(1, members // count)
    windows = 2 * local
    piece = tall // members
    steps = count // CHUNK
    chips = members // 2
    tables = build_tables(points, members)
    f32, bf16 = jnp.float32, jnp.bfloat16

    pieces = orbitals.reshape(count, 2, planes, tiles, LANES).transpose(0, 1, 3, 2, 4)
    pieces = pieces.reshape(count, 4, piece, LANES)

    smem = pl.BlockSpec(memory_space=pltpu.SMEM)
    vmem = pl.BlockSpec(memory_space=pltpu.VMEM)
    anywhere = pl.BlockSpec(memory_space=pl.ANY)
    dims = (local, bands, members, groups, points, planes)
    dma = pltpu.SemaphoreType.DMA
    out, matrix, energy = pl.pallas_call(
        functools.partial(exchange_kernel, dims),
        out_shape=(jax.ShapeDtypeStruct((count, 2, 2, piece, LANES), f32),
                   jax.ShapeDtypeStruct((local, 2, bands, bands), f32),
                   jax.ShapeDtypeStruct((1, 1), f32)),
        in_specs=[smem, smem, vmem, vmem] + [anywhere] * 5,
        out_specs=(vmem, vmem, smem),
        scratch_shapes=[
            pltpu.VMEM((2 * count, 2, chips, 4, piece, LANES), bf16),
            pltpu.VMEM(tables[0].shape, bf16), pltpu.VMEM(tables[1].shape, bf16),
            pltpu.VMEM(tables[2].shape, bf16), pltpu.VMEM(tables[3].shape, bf16),
            pltpu.VMEM(tables[4].shape, f32),
            pltpu.VMEM((local, windows, points, width), f32),
            pltpu.VMEM((2, 2, chips, local, points, width), f32),
            pltpu.VMEM((windows, 2 * tall, LANES), f32),
            pltpu.VMEM((rows, 2, 2, tall, LANES), f32),
            pltpu.VMEM((rows, 2, 2, tall, LANES), f32),
            pltpu.VMEM((share * count if share > 1 else 1, 2, 2, piece, LANES), f32),
            pltpu.VMEM((rows, 2, bands, LANES), f32),
            pltpu.VMEM((bands, LANES), f32),
            pltpu.VMEM((members, bands, LANES), f32),
            pltpu.VMEM((bands, LANES), f32),
            pltpu.VMEM((groups, bands, LANES), f32),
            dma((5,)), dma((4,)),
            dma((2 * chips - 2,)), dma((steps,)), dma((1,)), dma((steps,)), dma((steps,)), dma((1,)), dma((1,)),
            dma((chips - 1,)), dma((steps,)), dma((steps,)), dma((steps,)),
            dma((2, chips - 1)), dma((2,)), dma((2,)), dma((2,)),
            dma((rows, members - 1)), dma((rows, members - 1)), dma((members - 1,)), dma((members - 1,)),
            dma((groups - 1,)), dma((groups - 1,)),
        ],
        compiler_params=pltpu.CompilerParams(vmem_limit_bytes=56 * 2 ** 20, collective_id=0, has_side_effects=True),
        name="exchange",
    )(band_counts, pair_slot, pieces, kernel, *[jnp.asarray(table) for table in tables])
    out = out.reshape(local, bands, 2, tiles, planes, LANES).transpose(0, 1, 2, 4, 3, 5)
    return out.reshape(local, bands, 2, planes, columns), matrix, energy.reshape(())


def solution(mesh):
    in_specs = (P("ka", None, None, "ga", None), P(), P(), P(None, None, "ga"))
    out_specs = (P("ka", None, None, "ga", None), P("ka", None, None, None), P())
    return jax.shard_map(
        on_device, mesh=mesh, in_specs=in_specs, out_specs=out_specs, check_vma=False
    )
```

```python
import functools

import jax
import jax.numpy as jnp
import numpy as np
from jax import lax
from jax.experimental import pallas as pl
from jax.experimental.pallas import tpu as pltpu
from jax.sharding import PartitionSpec as P

LANES = 128
RADIX = 4
CHUNK = 2
LEAD = 3
SPLIT = 6
MESH = pl.DeviceIdType.MESH


def split_np(matrix):
    high = matrix.astype(np.float32).astype(jnp.bfloat16)
    low = (matrix - high.astype(np.float64)).astype(np.float32).astype(jnp.bfloat16)
    return high, low


def real_form(matrix):
    return np.block([[matrix.real, -matrix.imag], [matrix.imag, matrix.real]])


def build_tables(points, members):
    wide = LANES // points
    quads = points // (2 * wide)
    planes = points // members
    dft = np.exp(-2j * np.pi * np.outer(np.arange(points), np.arange(points)) / points)
    member_of = np.arange(members).reshape(members // 2, 2).T.reshape(-1)
    x_of = (member_of[:, None] * planes + np.arange(planes)[None, :]).reshape(members, 1, planes)
    deep = 2 * quads // RADIX
    b_of = np.arange(deep).reshape(1, deep, 1)
    x_of, b_of = (np.broadcast_to(v, (members, deep, planes)).reshape(-1) for v in (x_of, b_of))
    gx = np.tile(np.arange(points), deep)
    high_freq = np.repeat(np.arange(deep), points)
    left, left_back = [], []
    for c in range(RADIX):
        phase = np.outer(gx, x_of) / points + np.outer(c + RADIX * high_freq, b_of) / (2 * quads)
        forward = np.exp(-2j * np.pi * phase)
        high, low = split_np(real_form(forward))
        left.append(np.concatenate([high, high, low], axis=1))
        high, low = split_np(real_form(np.conj(forward).T))
        left_back.append(np.concatenate([high, high, low], axis=1))
    small = np.exp(-2j * np.pi * np.outer(np.arange(wide), np.arange(wide)) / wide)
    lane = np.kron(small, dft)
    right = []
    for matrix in (lane, np.conj(lane)):
        high, low = split_np(real_form(matrix).T)
        right.append(np.concatenate([high, low, high], axis=0))
    low_freq = (np.arange(RADIX)[:, None] + RADIX * np.arange(deep)[None, :]).reshape(-1)
    y0 = np.repeat(np.arange(wide), points)
    twiddle = np.exp(-2j * np.pi * np.outer(low_freq, y0) / points)
    twiddle = np.stack([twiddle.real, twiddle.imag]).astype(np.float32)
    return np.stack(left), np.stack(left_back), right[0], right[1], twiddle


def split(values):
    high = values.astype(jnp.bfloat16)
    low = (values - high.astype(jnp.float32)).astype(jnp.bfloat16)
    return high, low


def exchange_kernel(dims, counts, slots, pieces, kernel, left_in, left_back_in, right_in, right_back_in, twiddle_in,
                    out, matrix, energy,
                    block, left, left_back, right, right_back, twiddle, staged, raw, multiplier,
                    own, total, arrived, lanes_of, mail, mails, note, notes,
                    table_sem, local_sem, z_send, z_recv, r_send, d_send, d_recv, xo_send, xo_recv, x_send, x_recv,
                    p_send, p_recv, kz_send, kz_recv, kd_send, kd_recv, o_send, o_recv, m_send, m_recv, e_send, e_recv):
    local, bands, members, groups, points, planes = dims
    orbitals = local * bands
    chips = members // 2
    rows = max(1, orbitals // members)
    share = max(1, members // orbitals)
    landing = out if share == 1 else arrived
    windows = 2 * local
    steps = orbitals // CHUNK
    wide = LANES // points
    quads = points // (2 * wide)
    tall = quads * points
    deep = 2 * quads // RADIX
    low = deep * points
    piece = tall // members
    held = points // members
    volume = float(points ** 3)
    ready = max(1, 2 * rows // CHUNK)
    lead = min(max(LEAD, ready), steps)
    late = SPLIT if rows > 1 else 0
    paired = steps - max(late, lead)
    turns = 2 * steps - late
    relayed = 2 < chips <= 4

    me = lax.axis_index("ga")
    group = lax.axis_index("ka")
    core, chip = lax.rem(me, 2), lax.div(me, 2)
    partner = chip * 2 + 1 - core
    after = lax.rem(group + 1, groups)

    def row_of(member):
        return lax.div(member, share) * rows

    def start_of(at):
        return lax.div(row_of(at * 2), CHUNK)

    def chunk_at(at, j):
        rising = lax.rem(start_of(at) + j, steps)
        falling = lax.rem(start_of(at) + ready - 1 - j + 2 * steps, steps)
        return jnp.where(at < chips // 2, rising, falling) * CHUNK

    def chunk_of(at, j):
        return pl.ds(chunk_at(at, j), CHUNK)

    first_row = row_of(me)
    own_local = lax.div(first_row, bands)
    window_kpoints = [lax.rem(group + groups - w // local, groups) * local + w % local for w in range(windows)]

    def remote(src, dst, send, recv, **where):
        return pltpu.make_async_remote_copy(src_ref=src, dst_ref=dst, send_sem=send, recv_sem=recv,
                                            device_id=where, device_id_type=MESH)

    barrier = pltpu.get_barrier_semaphore()
    for d in range(1, members):
        pl.semaphore_signal(barrier, inc=1, device_id={"ga": lax.rem(me + d, members)}, device_id_type=MESH)
    for d in range(1, groups):
        pl.semaphore_signal(barrier, inc=1, device_id={"ka": lax.rem(group + d, groups)}, device_id_type=MESH)

    table_copies = [pltpu.make_async_copy(src, dst, table_sem.at[i]) for i, (src, dst) in enumerate(
        [(left_in, left), (left_back_in, left_back), (right_in, right), (right_back_in, right_back),
         (twiddle_in, twiddle)])]
    place = pltpu.make_async_copy(pieces, block.at[pl.ds(0, orbitals), core, chip], local_sem.at[0])
    place.start()
    for l in range(local):
        for w in range(windows):
            staged[l, w] = kernel[slots[group * local + l, window_kpoints[w]]] * (1.0 / volume)

    pl.semaphore_wait(barrier, members + groups - 2)

    offsets = [d for d in range(1 - chips, chips) if d != 0]
    ordered = sorted(offsets, key=lambda d: -abs(d))

    def z_copy(j, d):
        chunk = chunk_of(chip + d, j)
        return remote(pieces.at[chunk], block.at[chunk, core, chip], z_send.at[offsets.index(d)], z_recv.at[j],
                      ga=(chip + d) * 2 + core)

    def inside(d):
        return (chip + d >= 0) & (chip + d < chips)

    def far(d):
        return relayed and abs(d) == chips - 1

    def z_start(j, stop):
        for d in ordered:
            @pl.when(inside(d) & (j < (ready if far(d) else steps)))
            def _():
                z_copy(j, d).start()
        return stop

    def kz_copy(half, d):
        at = lax.rem(chip + d, chips)
        part = pl.ds(half * local, local)
        return remote(staged.at[lax.div(row_of(at * 2), bands), part], raw.at[half, core, chip],
                      kz_send.at[half, d - 1], kz_recv.at[half], ga=at * 2 + core)

    def relay_copy(j):
        low = chip == 1
        end, origin = jnp.where(low, 0, chips - 1), jnp.where(low, chips - 1, 0)
        chunk = chunk_of(end, j)
        here = block.at[chunk, core, origin]
        return remote(here, here, r_send.at[0], z_recv.at[j], ga=end * 2 + core)

    xo_copy = remote(pieces, block.at[pl.ds(orbitals, orbitals), core, chip], xo_send.at[0], xo_recv.at[0], ka=after)
    for d in range(1, chips):
        kz_copy(0, d).start()
    for j in range(ready):
        z_start(j, 0)
    xo_copy.start()
    for j in range(ready, lead):
        z_start(j, 0)
    for d in range(1, chips):
        kz_copy(1, d).start()
    lax.fori_loop(lead, steps, z_start, 0)
    for copy in table_copies:
        copy.start()
    kplaces = [pltpu.make_async_copy(staged.at[own_local, pl.ds(half * local, local)], raw.at[half, core, chip],
                                     local_sem.at[1 + half]) for half in range(2)]
    for copy in kplaces:
        copy.start()

    def d_copy(j):
        here = block.at[chunk_of(chip, j), core]
        return remote(here, here, d_send.at[j], d_recv.at[j], ga=partner)

    def x_copy(j, d):
        chunk = chunk_at(chip, j)
        at = lax.rem(chip + d, chips)
        return remote(block.at[pl.ds(chunk, CHUNK), core, at], block.at[pl.ds(orbitals + chunk, CHUNK), core, at],
                      x_send.at[d - 1], x_recv.at[j], ka=after)

    def p_copy(j):
        chunk = chunk_at(chip, j)
        here = block.at[pl.ds(orbitals + chunk, CHUNK), core]
        return remote(here, here, p_send.at[j], p_recv.at[j], ga=partner)

    def wait_for(dst, sem):
        pltpu.make_async_copy(dst, dst, sem).wait()

    def arrived_z(sem):
        wait_for(block.at[pl.ds(0, CHUNK), 0, pl.ds(0, chips - 1)], sem)

    def pass_own(j):
        arrived_z(z_recv.at[j])
        if relayed:
            @pl.when(((chip == 1) | (chip == chips - 2)) & (j + ready < steps))
            def _():
                relay_copy(j + ready).start()
        d_copy(j).start()
        for d in range(1, chips):
            x_copy(j, d).start()

    def kd_copy(half):
        return remote(raw.at[half, core], raw.at[half, core], kd_send.at[half], kd_recv.at[half], ga=partner)

    def pass_kernel(half):
        kplaces[half].wait()
        wait_for(raw.at[half, 0, pl.ds(0, chips - 1)], kz_recv.at[half])
        kd_copy(half).start()

    total[...] = jnp.zeros_like(total)
    place.wait()
    pass_kernel(0)

    each = points // members

    def lay_out(half):
        kd_copy(half).wait_recv()
        for l in range(local):
            for c in range(RADIX):
                for q in range(deep):
                    parts = []
                    for a in range(wide):
                        gy = a * 2 * quads + c + RADIX * q
                        at = gy // each
                        value = raw[half, at % 2, at // 2, l]
                        parts.append(value[:, (gy % each) * points:(gy % each + 1) * points])
                    multiplier[half * local + l, (c * deep + q) * points:(c * deep + q + 1) * points, :] = (
                        jnp.concatenate(parts, axis=1))

    pass_own(0)
    lay_out(0)
    for j in range(1, ready):
        pass_own(j)
    for copy in table_copies:
        copy.wait()

    def load(slot, part, h):
        value = block[slot, :, :, part * 2 + h]
        return value.astype(jnp.float32).reshape(tall, LANES)

    for j in range(ready):
        d_copy(j).wait_recv()
    for r in range(rows):
        for part in range(2):
            for h in range(2):
                own[r, part, h] = load(first_row + r, part, h)

    def rotate(real_part, imag_part, c, sign):
        cos = twiddle[0, c * deep:(c + 1) * deep, :].reshape(deep, 1, LANES)
        sin = twiddle[1, c * deep:(c + 1) * deep, :].reshape(deep, 1, LANES) * sign
        real_part = real_part.reshape(deep, points, LANES)
        imag_part = imag_part.reshape(deep, points, LANES)
        new_real = real_part * cos - imag_part * sin
        new_imag = imag_part * cos + real_part * sin
        return new_real.reshape(low, LANES), new_imag.reshape(low, LANES)

    def quarters(value):
        value = value.reshape(members, 2, piece // 2, LANES)
        return [value[:, n].reshape(low, LANES) for n in range(2)]

    def joined(first, second):
        shape = (members, 1, piece // 2, LANES)
        return jnp.concatenate([first.reshape(shape), second.reshape(shape)], axis=1).reshape(tall, LANES)

    def dot(a, b):
        return jnp.dot(a, b, preferred_element_type=jnp.float32)

    def from_left(table, values):
        high, low = split(values)
        return dot(table, jnp.concatenate([high, low, high], axis=0))

    def from_right(values, table):
        high, low = split(values)
        return dot(jnp.concatenate([high, high, low], axis=1), table)

    def turn_of(t):
        u = t - lead
        middle = (u >= 0) & (u < 2 * paired)
        back = jnp.where(middle, 1 - lax.rem(jnp.maximum(u, 0), 2), jnp.where(t - paired < steps, 0, 1))
        half = lax.div(jnp.maximum(u, 0), 2)
        index = jnp.where(u < 0, t, jnp.where(middle, jnp.where(back == 1, half, lead + half),
                                              jnp.where(t - paired < steps, t - paired, t - steps)))
        return back, index

    def partner_of(back, index, i):
        orbital = chunk_at(chip, index) + i
        slot = back * orbitals + orbital
        at_local, band = lax.div(orbital, bands), lax.rem(orbital, bands)
        w = back * local + at_local
        kpoint = lax.rem(group + groups - back, groups) * local + at_local
        keep = jnp.where(band < counts[kpoint], 1.0, 0.0).astype(jnp.float32)
        if share > 1:
            keep = keep * jnp.where(lax.rem(w, share) == lax.rem(me, share), 1.0, 0.0).astype(jnp.float32)
        return slot, w, keep

    def loads(item):
        held_ = {}
        for (slot, _, _), _ in item:
            if id(slot) not in held_:
                held_[id(slot)] = [[load(slot, part, h) for h in range(2)] for part in range(2)]
        return [held_[id(slot)] for (slot, _, _), _ in item]

    def first_stage(item):
        inputs = [[] for _ in range(RADIX)]
        for other, (_, r) in zip(loads(item), item):
            real, imag = [], []
            for h in range(2):
                real += quarters(own[r, 0, h] * other[0][h] + own[r, 1, h] * other[1][h])
                imag += quarters(own[r, 1, h] * other[0][h] - own[r, 0, h] * other[1][h])
            even = [[v[0] + v[2], v[1] + v[3]] for v in (real, imag)]
            odd = [[v[0] - v[2], v[1] - v[3]] for v in (real, imag)]
            inputs[0].append(jnp.concatenate([even[0][0] + even[0][1], even[1][0] + even[1][1]], axis=0))
            inputs[2].append(jnp.concatenate([even[0][0] - even[0][1], even[1][0] - even[1][1]], axis=0))
            inputs[1].append(jnp.concatenate([odd[0][0] + odd[1][1], odd[1][0] - odd[0][1]], axis=0))
            inputs[3].append(jnp.concatenate([odd[0][0] - odd[1][1], odd[1][0] + odd[0][1]], axis=0))
        return [from_left(left[c], jnp.concatenate(inputs[c], axis=1)) for c in range(RADIX)]

    def second_stage(spectra):
        result = []
        for p in range(2):
            turned = []
            for c in range(p * RADIX // 2, (p + 1) * RADIX // 2):
                for n in range(spectra[c].shape[1] // LANES):
                    cut = spectra[c][:, n * LANES:(n + 1) * LANES]
                    turned.append(jnp.concatenate(rotate(cut[:low], cut[low:], c, 1.0), axis=1))
            result.append(from_right(jnp.concatenate(turned, axis=0), right[...]))
        return result

    def third_stage(item, full):
        result = []
        for p in range(2):
            weighted = []
            for n in range(RADIX // 2):
                c = p * RADIX // 2 + n
                chosen = {}
                for i, ((slot, w, keep), _) in enumerate(item):
                    if id(slot) not in chosen:
                        value = multiplier[w, c * low:(c + 1) * low, :] * keep
                        chosen[id(slot)] = jnp.concatenate([value, value], axis=1)
                    at = n * len(item) + i
                    weighted.append(full[p][at * low:(at + 1) * low] * chosen[id(slot)])
            result.append(from_right(jnp.concatenate(weighted, axis=0), right_back[...]))
        return result

    def fourth_stage(item, full):
        values = []
        for p in range(2):
            for n in range(RADIX // 2):
                c = p * RADIX // 2 + n
                back_c = []
                for i in range(len(item)):
                    at = n * len(item) + i
                    cut = full[p][at * low:(at + 1) * low]
                    back_c.append(jnp.concatenate(rotate(cut[:, :LANES], cut[:, LANES:], c, -1.0), axis=0))
                values.append(from_left(left_back[c], jnp.concatenate(back_c, axis=1)))
        return values

    def last_stage(item, values):
        for i, (other, (_, r)) in enumerate(zip(loads(item), item)):
            cut = [value[:, i * LANES:(i + 1) * LANES] for value in values]
            real, imag = [v[:low] for v in cut], [v[low:] for v in cut]
            even = [[v[0] + v[2], v[1] + v[3]] for v in (real, imag)]
            odd = [[v[0] - v[2], v[1] - v[3]] for v in (real, imag)]
            real = [even[0][0] + even[0][1], odd[0][0] - odd[1][1], even[0][0] - even[0][1], odd[0][0] + odd[1][1]]
            imag = [even[1][0] + even[1][1], odd[1][0] + odd[0][1], even[1][0] - even[1][1], odd[1][0] - odd[0][1]]
            for h in range(2):
                real_part = joined(real[2 * h], real[2 * h + 1])
                imag_part = joined(imag[2 * h], imag[2 * h + 1])
                total[r, 0, h] += other[0][h] * real_part - other[1][h] * imag_part
                total[r, 1, h] += other[0][h] * imag_part + other[1][h] * real_part

    def work(a, b):
        va = first_stage(a)
        vb = first_stage(b)
        va = second_stage(va)
        vb = second_stage(vb)
        va = third_stage(a, va)
        vb = third_stage(b, vb)
        va = fourth_stage(a, va)
        vb = fourth_stage(b, vb)
        last_stage(a, va)
        last_stage(b, vb)

    def pass_back(j):
        wait_for(block.at[pl.ds(0, CHUNK), 0, pl.ds(0, chips - 1)], x_recv.at[j])
        p_copy(j).start()

    def step_body(step, carry):
        back, index = turn_of(step)
        next_back, next_index = turn_of(step + 1)

        @pl.when((next_back == 0) & (next_index >= ready))
        def _():
            pass_own(next_index)

        @pl.when(step == lead - 1)
        def _():
            xo_copy.wait_recv()
            pass_kernel(1)

        @pl.when((next_back == 1) & (step + 1 < turns))
        def _():
            pass_back(next_index)

        if late:
            @pl.when((step >= turns - late + 1) & (step + 1 < turns + late))
            def _():
                pass_back(step - turns + late - 1 + steps - late)

        @pl.when((back == 0) & (index >= ready))
        def _():
            d_copy(index).wait_recv()

        @pl.when(step == lead)
        def _():
            lay_out(1)

        @pl.when(back == 1)
        def _():
            p_copy(index).wait_recv()

        partners = [partner_of(back, index, i) for i in range(CHUNK)]
        work(*[[(partner, r) for r in range(rows)] for partner in partners])
        return carry

    lax.fori_loop(0, turns, step_body, 0)

    def seat(member):
        return lax.rem(member, 2) * chips + lax.div(member, 2)

    def o_copy(d, r):
        to = lax.rem(me + d, members)
        return remote(total.at[r, :, :, pl.ds(pl.multiple_of(seat(to) * piece, piece), piece)],
                      landing.at[lax.rem(me, share) * orbitals + first_row + r], o_send.at[r, d - 1], o_recv.at[r, d - 1],
                      ga=to)

    if late:
        pass_back(steps - 1)

    def row_body(r, carry):
        def turn(q, carry):
            first = steps - late + q * 2

            @pl.when(r == 0)
            def _():
                for n in range(2):
                    p_copy(first + n).wait_recv()

            partners = [[partner_of(1, first + n, i) for i in range(CHUNK)] for n in range(2)]
            work(*[[(partner, r) for partner in pair] for pair in partners])
            return carry

        lax.fori_loop(0, late // 2, turn, 0)
        for d in range(1, members):
            o_copy(d, r).start()
        return carry

    if late:
        lax.fori_loop(0, rows, row_body, 0)
    else:
        for r in range(rows):
            for d in range(1, members):
                o_copy(d, r).start()

    def project(a, carry):
        for r in range(rows):
            real_sum = jnp.zeros((tall, LANES), jnp.float32)
            imag_sum = jnp.zeros((tall, LANES), jnp.float32)
            for h in range(2):
                first, second = load(own_local * bands + a, 0, h), load(own_local * bands + a, 1, h)
                real_sum += first * total[r, 0, h] + second * total[r, 1, h]
                imag_sum += first * total[r, 1, h] - second * total[r, 0, h]
            lanes_of[r, 0, pl.ds(a, 1)] = jnp.sum(real_sum, axis=0, keepdims=True)
            lanes_of[r, 1, pl.ds(a, 1)] = jnp.sum(imag_sum, axis=0, keepdims=True)
        return carry

    lax.fori_loop(0, bands, project, 0)
    lane = lax.broadcasted_iota(jnp.int32, (bands, LANES), 1)
    level = lax.broadcasted_iota(jnp.int32, (bands, LANES), 0)
    entry = 2 * local * bands
    letter = jnp.zeros((bands, LANES), jnp.float32)
    for r in range(rows):
        at_band = lax.rem(first_row, bands) + r
        filled = jnp.where(at_band < counts[group * local + own_local], 1.0, 0.0).astype(jnp.float32)
        for part in range(2):
            value = jnp.sum(lanes_of[r, part], axis=1, keepdims=True) * (-1.0 / (groups * local * volume))
            letter = jnp.where(lane == (own_local * 2 + part) * bands + at_band, value, letter)
            if part == 0:
                term = jnp.where(level == at_band, value, 0.0) * (filled / (2.0 * groups * local))
                letter = letter + jnp.where(lane == entry, term, 0.0)
    mail[...] = letter
    mails[me] = letter

    def m_copy(d):
        to = lax.rem(me + d, members)
        return remote(mail, mails.at[me], m_send.at[d - 1], m_recv.at[d - 1], ga=to)

    for d in range(1, members):
        m_copy(d).start()

    own_part = pltpu.make_async_copy(total.at[:, :, :, pl.ds(pl.multiple_of(seat(me) * piece, piece), piece)],
                                     landing.at[pl.ds(lax.rem(me, share) * orbitals + first_row, rows)], local_sem.at[3])
    own_part.start()
    for d in range(1, members):
        m_copy(d).wait_recv()
    summed = jnp.sum(mails[...], axis=0)
    for l in range(local):
        for part in range(2):
            begin = (l * 2 + part) * bands
            matrix[l, part] = summed[:, begin:begin + bands]
    mine = jnp.where(lane == entry, summed, 0.0)
    note[...] = mine
    notes[group] = mine

    def e_copy(d):
        to = lax.rem(group + d, groups)
        return remote(note, notes.at[group], e_send.at[d - 1], e_recv.at[d - 1], ka=to)

    for d in range(1, groups):
        e_copy(d).start()

    for d in offsets:
        @pl.when(inside(d))
        def _():
            wait_for(pieces.at[pl.ds(0, ready * CHUNK)] if far(d) else pieces, z_send.at[offsets.index(d)])
    if relayed:
        @pl.when((chip == 1) | (chip == chips - 2))
        def _():
            wait_for(pieces.at[pl.ds(0, (steps - ready) * CHUNK)], r_send.at[0])
    for d in range(1, chips):
        wait_for(pieces, x_send.at[d - 1])
        kz_copy(0, d).wait_send()
        kz_copy(1, d).wait_send()
    kd_copy(0).wait_send()
    kd_copy(1).wait_send()
    xo_copy.wait_send()

    def drain(j, carry):
        d_copy(j).wait_send()
        p_copy(j).wait_send()
        return carry

    lax.fori_loop(0, steps, drain, 0)
    own_part.wait()
    for r in range(rows):
        for d in range(1, members):
            o_copy(d, r).wait_recv()

    if share > 1:
        def add_up(o, carry):
            value = arrived[o]
            for n in range(1, share):
                value = value + arrived[n * orbitals + o]
            out[o] = value
            return carry

        lax.fori_loop(0, orbitals, add_up, 0)
    for d in range(1, groups):
        e_copy(d).wait_recv()
    energy[0, 0] = jnp.sum(notes[...])

    for d in range(1, members):
        for r in range(rows):
            o_copy(d, r).wait_send()
        m_copy(d).wait_send()
    for d in range(1, groups):
        e_copy(d).wait_send()


def on_device(orbitals, band_counts, pair_slot, kernel):
    local, bands, _, planes, columns = orbitals.shape
    slots, points, width = kernel.shape
    members = lax.axis_size("ga")
    groups = lax.axis_size("ka")
    wide = LANES // points
    quads = points // (2 * wide)
    tall = quads * points
    tiles = columns // LANES
    count = local * bands
    rows = max(1, count // members)
    share = max(1, members // count)
    windows = 2 * local
    piece = tall // members
    steps = count // CHUNK
    chips = members // 2
    tables = build_tables(points, members)
    f32, bf16 = jnp.float32, jnp.bfloat16

    pieces = orbitals.reshape(count, 2, planes, tiles, LANES).transpose(0, 1, 3, 2, 4)
    pieces = pieces.reshape(count, 4, piece, LANES)

    smem = pl.BlockSpec(memory_space=pltpu.SMEM)
    vmem = pl.BlockSpec(memory_space=pltpu.VMEM)
    anywhere = pl.BlockSpec(memory_space=pl.ANY)
    dims = (local, bands, members, groups, points, planes)
    dma = pltpu.SemaphoreType.DMA
    out, matrix, energy = pl.pallas_call(
        functools.partial(exchange_kernel, dims),
        out_shape=(pltpu.VMEM((count, 2, 2, piece, LANES), f32),
                   pltpu.VMEM((local, 2, bands, bands), f32),
                   jax.ShapeDtypeStruct((1, 1), f32)),
        in_specs=[smem, smem, vmem, vmem] + [anywhere] * 5,
        out_specs=(vmem, vmem, smem),
        scratch_shapes=[
            pltpu.VMEM((2 * count, 2, chips, 4, piece, LANES), bf16),
            pltpu.VMEM(tables[0].shape, bf16), pltpu.VMEM(tables[1].shape, bf16),
            pltpu.VMEM(tables[2].shape, bf16), pltpu.VMEM(tables[3].shape, bf16),
            pltpu.VMEM(tables[4].shape, f32),
            pltpu.VMEM((local, windows, points, width), f32),
            pltpu.VMEM((2, 2, chips, local, points, width), f32),
            pltpu.VMEM((windows, 2 * tall, LANES), f32),
            pltpu.VMEM((rows, 2, 2, tall, LANES), f32),
            pltpu.VMEM((rows, 2, 2, tall, LANES), f32),
            pltpu.VMEM((share * count if share > 1 else 1, 2, 2, piece, LANES), f32),
            pltpu.VMEM((rows, 2, bands, LANES), f32),
            pltpu.VMEM((bands, LANES), f32),
            pltpu.VMEM((members, bands, LANES), f32),
            pltpu.VMEM((bands, LANES), f32),
            pltpu.VMEM((groups, bands, LANES), f32),
            dma((5,)), dma((4,)),
            dma((2 * chips - 2,)), dma((steps,)), dma((1,)), dma((steps,)), dma((steps,)), dma((1,)), dma((1,)),
            dma((chips - 1,)), dma((steps,)), dma((steps,)), dma((steps,)),
            dma((2, chips - 1)), dma((2,)), dma((2,)), dma((2,)),
            dma((rows, members - 1)), dma((rows, members - 1)), dma((members - 1,)), dma((members - 1,)),
            dma((groups - 1,)), dma((groups - 1,)),
        ],
        compiler_params=pltpu.CompilerParams(vmem_limit_bytes=56 * 2 ** 20, collective_id=0, has_side_effects=True),
        name="exchange",
    )(band_counts, pair_slot, pieces, kernel, *[jnp.asarray(table) for table in tables])
    out = out.reshape(local, bands, 2, tiles, planes, LANES).transpose(0, 1, 2, 4, 3, 5)
    return out.reshape(local, bands, 2, planes, columns) * (-1.0 / (local * groups)), matrix, energy.reshape(())


def solution(mesh):
    in_specs = (P("ka", None, None, "ga", None), P(), P(), P(None, None, "ga"))
    out_specs = (P("ka", None, None, "ga", None), P("ka", None, None, None), P())
    return jax.shard_map(
        on_device, mesh=mesh, in_specs=in_specs, out_specs=out_specs, check_vma=False
    )
```

```python
import functools

import jax
import jax.numpy as jnp
import numpy as np
from jax import lax
from jax.experimental import pallas as pl
from jax.experimental.pallas import tpu as pltpu
from jax.sharding import PartitionSpec as P

LANES = 128
RADIX = 4
CHUNK = 2
LEAD = 3
SPLIT = 6
MESH = pl.DeviceIdType.MESH


def split_np(matrix):
    high = matrix.astype(np.float32).astype(jnp.bfloat16)
    low = (matrix - high.astype(np.float64)).astype(np.float32).astype(jnp.bfloat16)
    return high, low


def real_form(matrix):
    return np.block([[matrix.real, -matrix.imag], [matrix.imag, matrix.real]])


def build_tables(points, members):
    wide = LANES // points
    quads = points // (2 * wide)
    planes = points // members
    dft = np.exp(-2j * np.pi * np.outer(np.arange(points), np.arange(points)) / points)
    member_of = np.arange(members).reshape(members // 2, 2).T.reshape(-1)
    x_of = (member_of[:, None] * planes + np.arange(planes)[None, :]).reshape(members, 1, planes)
    deep = 2 * quads // RADIX
    b_of = np.arange(deep).reshape(1, deep, 1)
    x_of, b_of = (np.broadcast_to(v, (members, deep, planes)).reshape(-1) for v in (x_of, b_of))
    gx = np.tile(np.arange(points), deep)
    high_freq = np.repeat(np.arange(deep), points)
    left, left_back = [], []
    for c in range(RADIX):
        phase = np.outer(gx, x_of) / points + np.outer(c + RADIX * high_freq, b_of) / (2 * quads)
        forward = np.exp(-2j * np.pi * phase)
        high, low = split_np(real_form(forward))
        left.append(np.concatenate([high, high, low], axis=1))
        high, low = split_np(real_form(np.conj(forward).T))
        left_back.append(np.concatenate([high, high, low], axis=1))
    small = np.exp(-2j * np.pi * np.outer(np.arange(wide), np.arange(wide)) / wide)
    lane = np.kron(small, dft)
    right = []
    for matrix in (lane, np.conj(lane)):
        high, low = split_np(real_form(matrix).T)
        right.append(np.concatenate([high, low, high], axis=0))
    low_freq = (np.arange(RADIX)[:, None] + RADIX * np.arange(deep)[None, :]).reshape(-1)
    y0 = np.repeat(np.arange(wide), points)
    twiddle = np.exp(-2j * np.pi * np.outer(low_freq, y0) / points)
    twiddle = np.stack([twiddle.real, twiddle.imag]).astype(np.float32)
    return np.stack(left), np.stack(left_back), right[0], right[1], twiddle


def split(values):
    high = values.astype(jnp.bfloat16)
    low = (values - high.astype(jnp.float32)).astype(jnp.bfloat16)
    return high, low


def exchange_kernel(dims, counts, slots, pieces, kernel, left_in, left_back_in, right_in, right_back_in, twiddle_in,
                    out, matrix, energy,
                    block, left, left_back, right, right_back, twiddle, staged, raw, multiplier,
                    own, total, arrived, lanes_of, mail, mails, note, notes,
                    table_sem, local_sem, z_send, z_recv, r_send, d_send, d_recv, xo_send, xo_recv, x_send, x_recv,
                    p_send, p_recv, kz_send, kz_recv, kd_send, kd_recv, o_send, o_recv, m_send, m_recv, e_send, e_recv):
    local, bands, members, groups, points, planes = dims
    orbitals = local * bands
    chips = members // 2
    rows = max(1, orbitals // members)
    share = max(1, members // orbitals)
    landing = out if share == 1 else arrived
    windows = 2 * local
    steps = orbitals // CHUNK
    wide = LANES // points
    quads = points // (2 * wide)
    tall = quads * points
    deep = 2 * quads // RADIX
    low = deep * points
    piece = tall // members
    held = points // members
    volume = float(points ** 3)
    ready = max(1, 2 * rows // CHUNK)
    lead = min(max(LEAD, ready), steps)
    late = SPLIT if rows > 1 else 0
    paired = steps - max(late, lead)
    turns = 2 * steps - late
    relayed = 2 < chips <= 4

    me = lax.axis_index("ga")
    group = lax.axis_index("ka")
    core, chip = lax.rem(me, 2), lax.div(me, 2)
    partner = chip * 2 + 1 - core
    after = lax.rem(group + 1, groups)

    def row_of(member):
        return lax.div(member, share) * rows

    def start_of(at):
        return lax.div(row_of(at * 2), CHUNK)

    def chunk_at(at, j):
        rising = lax.rem(start_of(at) + j, steps)
        falling = lax.rem(start_of(at) + ready - 1 - j + 2 * steps, steps)
        return jnp.where(at < chips // 2, rising, falling) * CHUNK

    def chunk_of(at, j):
        return pl.ds(chunk_at(at, j), CHUNK)

    first_row = row_of(me)
    own_local = lax.div(first_row, bands)
    window_kpoints = [lax.rem(group + groups - w // local, groups) * local + w % local for w in range(windows)]

    def remote(src, dst, send, recv, **where):
        return pltpu.make_async_remote_copy(src_ref=src, dst_ref=dst, send_sem=send, recv_sem=recv,
                                            device_id=where, device_id_type=MESH)

    barrier = pltpu.get_barrier_semaphore()
    for d in range(1, members):
        pl.semaphore_signal(barrier, inc=1, device_id={"ga": lax.rem(me + d, members)}, device_id_type=MESH)
    for d in range(1, groups):
        pl.semaphore_signal(barrier, inc=1, device_id={"ka": lax.rem(group + d, groups)}, device_id_type=MESH)

    table_copies = [pltpu.make_async_copy(src, dst, table_sem.at[i]) for i, (src, dst) in enumerate(
        [(left_in, left), (left_back_in, left_back), (right_in, right), (right_back_in, right_back),
         (twiddle_in, twiddle)])]
    place = pltpu.make_async_copy(pieces, block.at[pl.ds(0, orbitals), core, chip], local_sem.at[0])
    place.start()
    for l in range(local):
        for w in range(windows):
            staged[l, w] = kernel[slots[group * local + l, window_kpoints[w]]] * (1.0 / volume)

    pl.semaphore_wait(barrier, members + groups - 2)

    offsets = [d for d in range(1 - chips, chips) if d != 0]
    ordered = sorted(offsets, key=lambda d: -abs(d))

    def z_copy(j, d):
        chunk = chunk_of(chip + d, j)
        return remote(pieces.at[chunk], block.at[chunk, core, chip], z_send.at[offsets.index(d)], z_recv.at[j],
                      ga=(chip + d) * 2 + core)

    def inside(d):
        return (chip + d >= 0) & (chip + d < chips)

    def far(d):
        return relayed and abs(d) == chips - 1

    def z_start(j, stop):
        for d in ordered:
            @pl.when(inside(d) & (j < (ready if far(d) else steps)))
            def _():
                z_copy(j, d).start()
        return stop

    def kz_copy(half, d):
        at = lax.rem(chip + d, chips)
        part = pl.ds(half * local, local)
        return remote(staged.at[lax.div(row_of(at * 2), bands), part], raw.at[half, core, chip],
                      kz_send.at[half, d - 1], kz_recv.at[half], ga=at * 2 + core)

    def relay_copy(j):
        low = chip == 1
        end, origin = jnp.where(low, 0, chips - 1), jnp.where(low, chips - 1, 0)
        chunk = chunk_of(end, j)
        here = block.at[chunk, core, origin]
        return remote(here, here, r_send.at[0], z_recv.at[j], ga=end * 2 + core)

    xo_copy = remote(pieces, block.at[pl.ds(orbitals, orbitals), core, chip], xo_send.at[0], xo_recv.at[0], ka=after)
    for j in range(ready):
        z_start(j, 0)
    for d in range(1, chips):
        kz_copy(0, d).start()
    xo_copy.start()
    for j in range(ready, lead):
        z_start(j, 0)
    for d in range(1, chips):
        kz_copy(1, d).start()
    lax.fori_loop(lead, steps, z_start, 0)
    for copy in table_copies:
        copy.start()
    kplaces = [pltpu.make_async_copy(staged.at[own_local, pl.ds(half * local, local)], raw.at[half, core, chip],
                                     local_sem.at[1 + half]) for half in range(2)]
    for copy in kplaces:
        copy.start()

    def d_copy(j):
        here = block.at[chunk_of(chip, j), core]
        return remote(here, here, d_send.at[j], d_recv.at[j], ga=partner)

    def x_copy(j, d):
        chunk = chunk_at(chip, j)
        at = lax.rem(chip + d, chips)
        return remote(block.at[pl.ds(chunk, CHUNK), core, at], block.at[pl.ds(orbitals + chunk, CHUNK), core, at],
                      x_send.at[d - 1], x_recv.at[j], ka=after)

    def p_copy(j):
        chunk = chunk_at(chip, j)
        here = block.at[pl.ds(orbitals + chunk, CHUNK), core]
        return remote(here, here, p_send.at[j], p_recv.at[j], ga=partner)

    def wait_for(dst, sem):
        pltpu.make_async_copy(dst, dst, sem).wait()

    def arrived_z(sem):
        wait_for(block.at[pl.ds(0, CHUNK), 0, pl.ds(0, chips - 1)], sem)

    def pass_own(j):
        arrived_z(z_recv.at[j])
        if relayed:
            @pl.when(((chip == 1) | (chip == chips - 2)) & (j + ready < steps))
            def _():
                relay_copy(j + ready).start()
        d_copy(j).start()
        for d in range(1, chips):
            x_copy(j, d).start()

    def kd_copy(half):
        return remote(raw.at[half, core], raw.at[half, core], kd_send.at[half], kd_recv.at[half], ga=partner)

    def pass_kernel(half):
        kplaces[half].wait()
        wait_for(raw.at[half, 0, pl.ds(0, chips - 1)], kz_recv.at[half])
        kd_copy(half).start()

    total[...] = jnp.zeros_like(total)
    place.wait()
    for j in range(ready):
        pass_own(j)
    pass_kernel(0)

    each = points // members

    def lay_out(half):
        kd_copy(half).wait_recv()
        for l in range(local):
            for c in range(RADIX):
                for q in range(deep):
                    parts = []
                    for a in range(wide):
                        gy = a * 2 * quads + c + RADIX * q
                        at = gy // each
                        value = raw[half, at % 2, at // 2, l]
                        parts.append(value[:, (gy % each) * points:(gy % each + 1) * points])
                    multiplier[half * local + l, (c * deep + q) * points:(c * deep + q + 1) * points, :] = (
                        jnp.concatenate(parts, axis=1))

    lay_out(0)
    for copy in table_copies:
        copy.wait()

    def load(slot, part, h):
        value = block[slot, :, :, part * 2 + h]
        return value.astype(jnp.float32).reshape(tall, LANES)

    for j in range(ready):
        d_copy(j).wait_recv()
    for r in range(rows):
        for part in range(2):
            for h in range(2):
                own[r, part, h] = load(first_row + r, part, h)

    def rotate(real_part, imag_part, c, sign):
        cos = twiddle[0, c * deep:(c + 1) * deep, :].reshape(deep, 1, LANES)
        sin = twiddle[1, c * deep:(c + 1) * deep, :].reshape(deep, 1, LANES) * sign
        real_part = real_part.reshape(deep, points, LANES)
        imag_part = imag_part.reshape(deep, points, LANES)
        new_real = real_part * cos - imag_part * sin
        new_imag = imag_part * cos + real_part * sin
        return new_real.reshape(low, LANES), new_imag.reshape(low, LANES)

    def quarters(value):
        value = value.reshape(members, 2, piece // 2, LANES)
        return [value[:, n].reshape(low, LANES) for n in range(2)]

    def joined(first, second):
        shape = (members, 1, piece // 2, LANES)
        return jnp.concatenate([first.reshape(shape), second.reshape(shape)], axis=1).reshape(tall, LANES)

    def dot(a, b):
        return jnp.dot(a, b, preferred_element_type=jnp.float32)

    def from_left(table, values):
        high, low = split(values)
        return dot(table, jnp.concatenate([high, low, high], axis=0))

    def from_right(values, table):
        high, low = split(values)
        return dot(jnp.concatenate([high, high, low], axis=1), table)

    def turn_of(t):
        u = t - lead
        middle = (u >= 0) & (u < 2 * paired)
        back = jnp.where(middle, 1 - lax.rem(jnp.maximum(u, 0), 2), jnp.where(t - paired < steps, 0, 1))
        half = lax.div(jnp.maximum(u, 0), 2)
        index = jnp.where(u < 0, t, jnp.where(middle, jnp.where(back == 1, half, lead + half),
                                              jnp.where(t - paired < steps, t - paired, t - steps)))
        return back, index

    def partner_of(back, index, i):
        orbital = chunk_at(chip, index) + i
        slot = back * orbitals + orbital
        at_local, band = lax.div(orbital, bands), lax.rem(orbital, bands)
        w = back * local + at_local
        kpoint = lax.rem(group + groups - back, groups) * local + at_local
        keep = jnp.where(band < counts[kpoint], 1.0, 0.0).astype(jnp.float32)
        if share > 1:
            keep = keep * jnp.where(lax.rem(w, share) == lax.rem(me, share), 1.0, 0.0).astype(jnp.float32)
        return slot, w, keep

    def loads(item):
        held_ = {}
        for (slot, _, _), _ in item:
            if id(slot) not in held_:
                held_[id(slot)] = [[load(slot, part, h) for h in range(2)] for part in range(2)]
        return [held_[id(slot)] for (slot, _, _), _ in item]

    def first_stage(item):
        inputs = [[] for _ in range(RADIX)]
        for other, (_, r) in zip(loads(item), item):
            real, imag = [], []
            for h in range(2):
                real += quarters(own[r, 0, h] * other[0][h] + own[r, 1, h] * other[1][h])
                imag += quarters(own[r, 1, h] * other[0][h] - own[r, 0, h] * other[1][h])
            even = [[v[0] + v[2], v[1] + v[3]] for v in (real, imag)]
            odd = [[v[0] - v[2], v[1] - v[3]] for v in (real, imag)]
            inputs[0].append(jnp.concatenate([even[0][0] + even[0][1], even[1][0] + even[1][1]], axis=0))
            inputs[2].append(jnp.concatenate([even[0][0] - even[0][1], even[1][0] - even[1][1]], axis=0))
            inputs[1].append(jnp.concatenate([odd[0][0] + odd[1][1], odd[1][0] - odd[0][1]], axis=0))
            inputs[3].append(jnp.concatenate([odd[0][0] - odd[1][1], odd[1][0] + odd[0][1]], axis=0))
        return [from_left(left[c], jnp.concatenate(inputs[c], axis=1)) for c in range(RADIX)]

    def second_stage(spectra):
        result = []
        for p in range(2):
            turned = []
            for c in range(p * RADIX // 2, (p + 1) * RADIX // 2):
                for n in range(spectra[c].shape[1] // LANES):
                    cut = spectra[c][:, n * LANES:(n + 1) * LANES]
                    turned.append(jnp.concatenate(rotate(cut[:low], cut[low:], c, 1.0), axis=1))
            result.append(from_right(jnp.concatenate(turned, axis=0), right[...]))
        return result

    def third_stage(item, full):
        result = []
        for p in range(2):
            weighted = []
            for n in range(RADIX // 2):
                c = p * RADIX // 2 + n
                chosen = {}
                for i, ((slot, w, keep), _) in enumerate(item):
                    if id(slot) not in chosen:
                        value = multiplier[w, c * low:(c + 1) * low, :] * keep
                        chosen[id(slot)] = jnp.concatenate([value, value], axis=1)
                    at = n * len(item) + i
                    weighted.append(full[p][at * low:(at + 1) * low] * chosen[id(slot)])
            result.append(from_right(jnp.concatenate(weighted, axis=0), right_back[...]))
        return result

    def fourth_stage(item, full):
        values = []
        for p in range(2):
            for n in range(RADIX // 2):
                c = p * RADIX // 2 + n
                back_c = []
                for i in range(len(item)):
                    at = n * len(item) + i
                    cut = full[p][at * low:(at + 1) * low]
                    back_c.append(jnp.concatenate(rotate(cut[:, :LANES], cut[:, LANES:], c, -1.0), axis=0))
                values.append(from_left(left_back[c], jnp.concatenate(back_c, axis=1)))
        return values

    def last_stage(item, values):
        for i, (other, (_, r)) in enumerate(zip(loads(item), item)):
            cut = [value[:, i * LANES:(i + 1) * LANES] for value in values]
            real, imag = [v[:low] for v in cut], [v[low:] for v in cut]
            even = [[v[0] + v[2], v[1] + v[3]] for v in (real, imag)]
            odd = [[v[0] - v[2], v[1] - v[3]] for v in (real, imag)]
            real = [even[0][0] + even[0][1], odd[0][0] - odd[1][1], even[0][0] - even[0][1], odd[0][0] + odd[1][1]]
            imag = [even[1][0] + even[1][1], odd[1][0] + odd[0][1], even[1][0] - even[1][1], odd[1][0] - odd[0][1]]
            for h in range(2):
                real_part = joined(real[2 * h], real[2 * h + 1])
                imag_part = joined(imag[2 * h], imag[2 * h + 1])
                total[r, 0, h] += other[0][h] * real_part - other[1][h] * imag_part
                total[r, 1, h] += other[0][h] * imag_part + other[1][h] * real_part

    def work(a, b):
        va = first_stage(a)
        vb = first_stage(b)
        va = second_stage(va)
        vb = second_stage(vb)
        va = third_stage(a, va)
        vb = third_stage(b, vb)
        va = fourth_stage(a, va)
        vb = fourth_stage(b, vb)
        last_stage(a, va)
        last_stage(b, vb)

    def pass_back(j):
        wait_for(block.at[pl.ds(0, CHUNK), 0, pl.ds(0, chips - 1)], x_recv.at[j])
        p_copy(j).start()

    def step_body(step, carry):
        back, index = turn_of(step)
        next_back, next_index = turn_of(step + 1)

        @pl.when((next_back == 0) & (next_index >= ready))
        def _():
            pass_own(next_index)

        @pl.when(step == lead - 1)
        def _():
            xo_copy.wait_recv()
            pass_kernel(1)

        @pl.when((next_back == 1) & (step + 1 < turns))
        def _():
            pass_back(next_index)

        if late:
            @pl.when((step >= turns - late + 1) & (step + 1 < turns + late))
            def _():
                pass_back(step - turns + late - 1 + steps - late)

        @pl.when((back == 0) & (index >= ready))
        def _():
            d_copy(index).wait_recv()

        @pl.when(step == lead)
        def _():
            lay_out(1)

        @pl.when(back == 1)
        def _():
            p_copy(index).wait_recv()

        partners = [partner_of(back, index, i) for i in range(CHUNK)]
        work(*[[(partner, r) for r in range(rows)] for partner in partners])
        return carry

    lax.fori_loop(0, turns, step_body, 0)

    def seat(member):
        return lax.rem(member, 2) * chips + lax.div(member, 2)

    def o_copy(d, r):
        to = lax.rem(me + d, members)
        return remote(total.at[r, :, :, pl.ds(pl.multiple_of(seat(to) * piece, piece), piece)],
                      landing.at[lax.rem(me, share) * orbitals + first_row + r], o_send.at[r, d - 1], o_recv.at[r, d - 1],
                      ga=to)

    if late:
        pass_back(steps - 1)

    def row_body(r, carry):
        def turn(q, carry):
            first = steps - late + q * 2

            @pl.when(r == 0)
            def _():
                for n in range(2):
                    p_copy(first + n).wait_recv()

            partners = [[partner_of(1, first + n, i) for i in range(CHUNK)] for n in range(2)]
            work(*[[(partner, r) for partner in pair] for pair in partners])
            return carry

        lax.fori_loop(0, late // 2, turn, 0)
        for d in range(1, members):
            o_copy(d, r).start()
        return carry

    if late:
        lax.fori_loop(0, rows, row_body, 0)
    else:
        for r in range(rows):
            for d in range(1, members):
                o_copy(d, r).start()

    def project(a, carry):
        for r in range(rows):
            real_sum = jnp.zeros((tall, LANES), jnp.float32)
            imag_sum = jnp.zeros((tall, LANES), jnp.float32)
            for h in range(2):
                first, second = load(own_local * bands + a, 0, h), load(own_local * bands + a, 1, h)
                real_sum += first * total[r, 0, h] + second * total[r, 1, h]
                imag_sum += first * total[r, 1, h] - second * total[r, 0, h]
            lanes_of[r, 0, pl.ds(a, 1)] = jnp.sum(real_sum, axis=0, keepdims=True)
            lanes_of[r, 1, pl.ds(a, 1)] = jnp.sum(imag_sum, axis=0, keepdims=True)
        return carry

    lax.fori_loop(0, bands, project, 0)
    lane = lax.broadcasted_iota(jnp.int32, (bands, LANES), 1)
    level = lax.broadcasted_iota(jnp.int32, (bands, LANES), 0)
    entry = 2 * local * bands
    letter = jnp.zeros((bands, LANES), jnp.float32)
    for r in range(rows):
        at_band = lax.rem(first_row, bands) + r
        filled = jnp.where(at_band < counts[group * local + own_local], 1.0, 0.0).astype(jnp.float32)
        for part in range(2):
            value = jnp.sum(lanes_of[r, part], axis=1, keepdims=True) * (-1.0 / (groups * local * volume))
            letter = jnp.where(lane == (own_local * 2 + part) * bands + at_band, value, letter)
            if part == 0:
                term = jnp.where(level == at_band, value, 0.0) * (filled / (2.0 * groups * local))
                letter = letter + jnp.where(lane == entry, term, 0.0)
    mail[...] = letter
    mails[me] = letter

    def m_copy(d):
        to = lax.rem(me + d, members)
        return remote(mail, mails.at[me], m_send.at[d - 1], m_recv.at[d - 1], ga=to)

    for d in range(1, members):
        m_copy(d).start()

    own_part = pltpu.make_async_copy(total.at[:, :, :, pl.ds(pl.multiple_of(seat(me) * piece, piece), piece)],
                                     landing.at[pl.ds(lax.rem(me, share) * orbitals + first_row, rows)], local_sem.at[3])
    own_part.start()
    for d in range(1, members):
        m_copy(d).wait_recv()
    summed = jnp.sum(mails[...], axis=0)
    for l in range(local):
        for part in range(2):
            begin = (l * 2 + part) * bands
            matrix[l, part] = summed[:, begin:begin + bands]
    mine = jnp.where(lane == entry, summed, 0.0)
    note[...] = mine
    notes[group] = mine

    def e_copy(d):
        to = lax.rem(group + d, groups)
        return remote(note, notes.at[group], e_send.at[d - 1], e_recv.at[d - 1], ka=to)

    for d in range(1, groups):
        e_copy(d).start()

    for d in offsets:
        @pl.when(inside(d))
        def _():
            wait_for(pieces.at[pl.ds(0, ready * CHUNK)] if far(d) else pieces, z_send.at[offsets.index(d)])
    if relayed:
        @pl.when((chip == 1) | (chip == chips - 2))
        def _():
            wait_for(pieces.at[pl.ds(0, (steps - ready) * CHUNK)], r_send.at[0])
    for d in range(1, chips):
        wait_for(pieces, x_send.at[d - 1])
        kz_copy(0, d).wait_send()
        kz_copy(1, d).wait_send()
    kd_copy(0).wait_send()
    kd_copy(1).wait_send()
    xo_copy.wait_send()

    def drain(j, carry):
        d_copy(j).wait_send()
        p_copy(j).wait_send()
        return carry

    lax.fori_loop(0, steps, drain, 0)
    own_part.wait()
    for r in range(rows):
        for d in range(1, members):
            o_copy(d, r).wait_recv()

    if share > 1:
        def add_up(o, carry):
            value = arrived[o]
            for n in range(1, share):
                value = value + arrived[n * orbitals + o]
            out[o] = value
            return carry

        lax.fori_loop(0, orbitals, add_up, 0)
    for d in range(1, groups):
        e_copy(d).wait_recv()
    energy[0, 0] = jnp.sum(notes[...])

    for d in range(1, members):
        for r in range(rows):
            o_copy(d, r).wait_send()
        m_copy(d).wait_send()
    for d in range(1, groups):
        e_copy(d).wait_send()


def on_device(orbitals, band_counts, pair_slot, kernel):
    local, bands, _, planes, columns = orbitals.shape
    slots, points, width = kernel.shape
    members = lax.axis_size("ga")
    groups = lax.axis_size("ka")
    wide = LANES // points
    quads = points // (2 * wide)
    tall = quads * points
    tiles = columns // LANES
    count = local * bands
    rows = max(1, count // members)
    share = max(1, members // count)
    windows = 2 * local
    piece = tall // members
    steps = count // CHUNK
    chips = members // 2
    tables = build_tables(points, members)
    f32, bf16 = jnp.float32, jnp.bfloat16

    pieces = orbitals.reshape(count, 2, planes, tiles, LANES).transpose(0, 1, 3, 2, 4)
    pieces = pieces.reshape(count, 4, piece, LANES)

    smem = pl.BlockSpec(memory_space=pltpu.SMEM)
    vmem = pl.BlockSpec(memory_space=pltpu.VMEM)
    anywhere = pl.BlockSpec(memory_space=pl.ANY)
    dims = (local, bands, members, groups, points, planes)
    dma = pltpu.SemaphoreType.DMA
    out, matrix, energy = pl.pallas_call(
        functools.partial(exchange_kernel, dims),
        out_shape=(pltpu.VMEM((count, 2, 2, piece, LANES), f32),
                   pltpu.VMEM((local, 2, bands, bands), f32),
                   jax.ShapeDtypeStruct((1, 1), f32)),
        in_specs=[smem, smem, vmem, vmem] + [anywhere] * 5,
        out_specs=(vmem, vmem, smem),
        scratch_shapes=[
            pltpu.VMEM((2 * count, 2, chips, 4, piece, LANES), bf16),
            pltpu.VMEM(tables[0].shape, bf16), pltpu.VMEM(tables[1].shape, bf16),
            pltpu.VMEM(tables[2].shape, bf16), pltpu.VMEM(tables[3].shape, bf16),
            pltpu.VMEM(tables[4].shape, f32),
            pltpu.VMEM((local, windows, points, width), f32),
            pltpu.VMEM((2, 2, chips, local, points, width), f32),
            pltpu.VMEM((windows, 2 * tall, LANES), f32),
            pltpu.VMEM((rows, 2, 2, tall, LANES), f32),
            pltpu.VMEM((rows, 2, 2, tall, LANES), f32),
            pltpu.VMEM((share * count if share > 1 else 1, 2, 2, piece, LANES), f32),
            pltpu.VMEM((rows, 2, bands, LANES), f32),
            pltpu.VMEM((bands, LANES), f32),
            pltpu.VMEM((members, bands, LANES), f32),
            pltpu.VMEM((bands, LANES), f32),
            pltpu.VMEM((groups, bands, LANES), f32),
            dma((5,)), dma((4,)),
            dma((2 * chips - 2,)), dma((steps,)), dma((1,)), dma((steps,)), dma((steps,)), dma((1,)), dma((1,)),
            dma((chips - 1,)), dma((steps,)), dma((steps,)), dma((steps,)),
            dma((2, chips - 1)), dma((2,)), dma((2,)), dma((2,)),
            dma((rows, members - 1)), dma((rows, members - 1)), dma((members - 1,)), dma((members - 1,)),
            dma((groups - 1,)), dma((groups - 1,)),
        ],
        compiler_params=pltpu.CompilerParams(vmem_limit_bytes=56 * 2 ** 20, collective_id=0, has_side_effects=True),
        name="exchange",
    )(band_counts, pair_slot, pieces, kernel, *[jnp.asarray(table) for table in tables])
    out = out.reshape(local, bands, 2, tiles, planes, LANES).transpose(0, 1, 2, 4, 3, 5)
    return out.reshape(local, bands, 2, planes, columns) * (-1.0 / (local * groups)), matrix, energy.reshape(())


def solution(mesh):
    in_specs = (P("ka", None, None, "ga", None), P(), P(), P(None, None, "ga"))
    out_specs = (P("ka", None, None, "ga", None), P("ka", None, None, None), P())
    return jax.shard_map(
        on_device, mesh=mesh, in_specs=in_specs, out_specs=out_specs, check_vma=False
    )
```
